32 devices in a mesh: dp: 2 (over x), tp: 4 (over z), sp: 4 (over y, core).
Axes of the slice: x: 2, y: 2, z: 4, core: 2. Of those that a mesh axis runs over, the one named last changes fastest.
Arguments:
- hidden: bfloat16 [4, 128, 2560], P(None, 'dp'), parts along dimension 1
- start_pos: int32 [128], P('dp'), parts along dimension 0
- k_cache: bfloat16 [128, 1024, 8, 128], P('dp', 'sp', 'tp'), parts along dimension 0
- v_cache: bfloat16 [128, 1024, 8, 128], P('dp', 'sp', 'tp'), parts along dimension 0
- w_q: bfloat16 [2560, 4096], P(None, 'tp')
- w_k: bfloat16 [2560, 1024], P(None, 'tp')
- w_v: bfloat16 [2560, 1024], P(None, 'tp')
- w_o: bfloat16 [4096, 2560], P('tp')
- w_gate: bfloat16 [2560, 9728], P(None, 'tp')
- w_up: bfloat16 [2560, 9728], P(None, 'tp')
- w_down: bfloat16 [9728, 2560], P('tp')
- attn_norm: bfloat16 [2560], replicated
- mlp_norm: bfloat16 [2560], replicated
- q_gain: bfloat16 [128], replicated
- k_gain: bfloat16 [128], replicated
Outputs:
- output 1: bfloat16 [4, 128, 2560], P(None, 'dp'), parts along dimension 1
- output 2: bfloat16 [128, 1024, 8, 128], P('dp', 'sp', 'tp'), parts along dimension 0
- output 3: bfloat16 [128, 1024, 8, 128], P('dp', 'sp', 'tp'), parts along dimension 0
There are 2 independent parts. The reference program is written for one: setup_inputs(seed, part) draws one part's arguments, and reference() takes and returns one part's arrays. A program takes and returns all parts, laid end to end along the dimension named above; an argument that names none is the same for every part.
All inputs are finite; a program needn't handle non-finite values.
Results may differ from the reference program's by a relative error of at most 0.00859188.
Values sent between devices are 32-bit elements.
A program may use at most 1 GiB of HBM per device.

```python
import math
import jax
import jax.numpy as jnp
from jax import lax

D_MODEL = 2560
HEADS = 32
KV_HEADS = 8
FFN_DIM = 9728
HEAD_DIM = 128
STEPS = 4
BATCH = 64
SEQ_DEV = 256
SEQ_LEN = 1024
ROPE_BASE = 1000000.0
NORM_EPS = 1e-06


def rms_scale(values, gain_vec):
    wide_vals = values.astype(jnp.float32)
    inv_rms = lax.rsqrt(jnp.mean(wide_vals * wide_vals, axis=-1, keepdims=True) + NORM_EPS)
    return wide_vals * inv_rms * gain_vec.astype(jnp.float32)


def apply_rope(vector, tok_pos):
    head_dim = vector.shape[-1]
    half_dim = head_dim // 2
    freqs = ROPE_BASE ** (-(jnp.arange(half_dim, dtype=jnp.float32) * (2.0 / head_dim)))
    angles = tok_pos.astype(jnp.float32)[:, None] * freqs[None, :]
    cos_tab = jnp.cos(angles)[:, None, :]
    sin_tab = jnp.sin(angles)[:, None, :]
    lower_half = vector[..., :half_dim]
    upper_half = vector[..., half_dim:]
    return jnp.concatenate([lower_half * cos_tab - upper_half * sin_tab, upper_half * cos_tab + lower_half * sin_tab], axis=-1)


def setup_inputs(seed: int = 0, part: int = 0) -> dict:
    w_keys = jax.random.split(jax.random.key(seed), 11)
    part_keys = jax.random.split(jax.random.fold_in(jax.random.key(seed + 1), part), 5)
    q_width = HEADS * HEAD_DIM
    kv_width = KV_HEADS * HEAD_DIM
    q_scale = math.sqrt(math.log(SEQ_LEN / 16.0))
    k_scale = math.sqrt(2.0 * math.log(SEQ_LEN)) / 1.5

    def normal_draw(key_in, shape, scale):
        return (jax.random.normal(key_in, shape, jnp.float32) * scale).astype(jnp.bfloat16)

    def gain_draw(key_in, shape, scale):
        return (scale * (1.0 + 0.2 * jax.random.normal(key_in, shape, jnp.float32))).astype(jnp.bfloat16)

    drawn_pos = jax.random.randint(part_keys[1], (BATCH,), SEQ_DEV, SEQ_LEN - STEPS + 1, dtype=jnp.int32)
    order = jax.random.permutation(part_keys[2], BATCH)
    start_pos = drawn_pos.at[order[0]].set(SEQ_LEN - STEPS).at[order[1]].set(SEQ_DEV)
    filled = (jnp.arange(SEQ_LEN)[None, :] < start_pos[:, None])[:, :, None, None]
    cache_shape = (BATCH, SEQ_LEN, KV_HEADS, HEAD_DIM)
    k_cache = jnp.where(filled, jax.random.normal(part_keys[3], cache_shape, jnp.float32), 0.0).astype(jnp.bfloat16)
    v_cache = jnp.where(filled, jax.random.normal(part_keys[4], cache_shape, jnp.float32), 0.0).astype(jnp.bfloat16)
    return {
        'hidden': normal_draw(part_keys[0], (STEPS, BATCH, D_MODEL), 1.0),
        'start_pos': start_pos,
        'k_cache': k_cache,
        'v_cache': v_cache,
        'w_q': normal_draw(w_keys[0], (D_MODEL, q_width), D_MODEL ** -0.5),
        'w_k': normal_draw(w_keys[1], (D_MODEL, kv_width), D_MODEL ** -0.5),
        'w_v': normal_draw(w_keys[2], (D_MODEL, kv_width), D_MODEL ** -0.5),
        'w_o': normal_draw(w_keys[3], (q_width, D_MODEL), 2.0 * q_width ** -0.5),
        'w_gate': normal_draw(w_keys[4], (D_MODEL, FFN_DIM), D_MODEL ** -0.5),
        'w_up': normal_draw(w_keys[5], (D_MODEL, FFN_DIM), D_MODEL ** -0.5),
        'w_down': normal_draw(w_keys[6], (FFN_DIM, D_MODEL), FFN_DIM ** -0.5),
        'attn_norm': gain_draw(w_keys[7], (D_MODEL,), 1.0),
        'mlp_norm': gain_draw(w_keys[8], (D_MODEL,), 1.0),
        'q_gain': gain_draw(w_keys[9], (HEAD_DIM,), q_scale),
        'k_gain': gain_draw(w_keys[10], (HEAD_DIM,), k_scale),
    }


def reference(hidden, start_pos, k_cache, v_cache, w_q, w_k, w_v, w_o, w_gate, w_up, w_down, attn_norm, mlp_norm, q_gain, k_gain):
    groups = HEADS // KV_HEADS
    score_scale = HEAD_DIM ** -0.5
    seq_pos = jnp.arange(SEQ_LEN)

    def attend_one(request):
        q_one, k_one, v_one, pos_one = request
        scores = jnp.einsum('kgh,lkh->kgl', q_one.astype(jnp.float32), k_one.astype(jnp.float32)) * score_scale
        scores = jnp.where(seq_pos <= pos_one, scores, -jnp.inf)
        probs = jax.nn.softmax(scores, axis=-1)
        return jnp.einsum('kgl,lkh->kgh', probs, v_one.astype(jnp.float32))

    def decode_step(caches, step_in):
        k_all, v_all = caches
        x_tok, step_idx = step_in
        tok_pos = start_pos + step_idx
        normed = rms_scale(x_tok, attn_norm).astype(jnp.bfloat16)
        q_raw = jnp.dot(normed, w_q, preferred_element_type=jnp.float32).reshape(BATCH, HEADS, HEAD_DIM)
        k_raw = jnp.dot(normed, w_k, preferred_element_type=jnp.float32).reshape(BATCH, KV_HEADS, HEAD_DIM)
        v_new = jnp.dot(normed, w_v, preferred_element_type=jnp.float32).astype(jnp.bfloat16).reshape(BATCH, KV_HEADS, HEAD_DIM)
        q_rot = apply_rope(rms_scale(q_raw, q_gain), tok_pos).astype(jnp.bfloat16).reshape(BATCH, KV_HEADS, groups, HEAD_DIM)
        k_new = apply_rope(rms_scale(k_raw, k_gain), tok_pos).astype(jnp.bfloat16)
        hit = (seq_pos[None, :] == tok_pos[:, None])[:, :, None, None]
        k_all = jnp.where(hit, k_new[:, None], k_all)
        v_all = jnp.where(hit, v_new[:, None], v_all)
        attn_vals = lax.map(attend_one, (q_rot, k_all, v_all, tok_pos))
        attn_in = attn_vals.reshape(BATCH, HEADS * HEAD_DIM).astype(jnp.bfloat16)
        attn_out = jnp.dot(attn_in, w_o, preferred_element_type=jnp.float32)
        residual = (x_tok.astype(jnp.float32) + attn_out).astype(jnp.bfloat16)
        mlp_in = rms_scale(residual, mlp_norm).astype(jnp.bfloat16)
        gate_act = jnp.dot(mlp_in, w_gate, preferred_element_type=jnp.float32)
        up_proj = jnp.dot(mlp_in, w_up, preferred_element_type=jnp.float32)
        mlp_act = (jax.nn.silu(gate_act) * up_proj).astype(jnp.bfloat16)
        down_out = jnp.dot(mlp_act, w_down, preferred_element_type=jnp.float32)
        out_tok = (residual.astype(jnp.float32) + down_out).astype(jnp.bfloat16)
        return (k_all, v_all), out_tok

    final_caches, outputs = lax.scan(decode_step, (k_cache, v_cache), (hidden, jnp.arange(STEPS)))
    return outputs, final_caches[0], final_caches[1]
```

```python
import functools
import jax
import jax.numpy as jnp
from jax import lax
from jax.experimental import pallas as pl
from jax.experimental.pallas import tpu as pltpu
from jax.sharding import PartitionSpec as P

ROPE_BASE = 1000000.0
NORM_EPS = 1e-06
NEG = -3.0e38
F32 = jnp.float32
BF16 = jnp.bfloat16
MESH = pl.DeviceIdType.MESH
STATS = 128
GROUP = 4
PIECE = 256
LAG = 2
VMEM_LIMIT = 66_900_000


def dot(a, b):
    return jnp.dot(a, b, preferred_element_type=F32)


def attn_kernel(start_ref, hid_ref, cos_ref, sin_ref, norm_ref, qg_ref, kg_ref, wq_ref, wk_ref, wv_ref, kc_ref, vc_ref,
                o_ref, ko_ref, vo_ref,
                hid, normed, wq, wk, wv, kbuf, vbuf, qs, ks, vs, ostage, thr, hid_sem, w_sem, in_sem, out_sem, o_sem):
    n_rows, d_model = hid.shape
    n_batch, rows_kv, hd = kbuf.shape
    n_steps = n_rows // n_batch
    heads = wq.shape[1] // hd
    kv = wk.shape[1] // hd
    seq = rows_kv // kv
    n_groups = n_batch // GROUP
    qrows = heads * n_steps
    blk_start = lax.axis_index('sp') * seq

    hid_cp = pltpu.make_async_copy(hid_ref, hid, hid_sem)
    hid_cp.start()
    n_q = wq.shape[1] // 256
    w_cps = []
    for i in range(n_q):
        w_cps.append(pltpu.make_async_copy(wq_ref.at[:, pl.ds(i * 256, 256)], wq.at[:, pl.ds(i * 256, 256)], w_sem.at[i]))
    w_cps.append(pltpu.make_async_copy(wk_ref, wk, w_sem.at[n_q]))
    w_cps.append(pltpu.make_async_copy(wv_ref, wv, w_sem.at[n_q + 1]))
    for cp in w_cps:
        cp.start()

    def cache_in(g, which):
        src, dst = ((kc_ref, kbuf), (vc_ref, vbuf))[which]
        rows = pl.ds(g * GROUP, GROUP)
        return pltpu.make_async_copy(src.at[rows], dst.at[rows], in_sem.at[which, g])

    def cache_out(g, which):
        src, dst = ((kbuf, ko_ref), (vbuf, vo_ref))[which]
        rows = pl.ds(g * GROUP, GROUP)
        return pltpu.make_async_copy(src.at[rows], dst.at[rows], out_sem.at[which, g])

    def o_out(g):
        rows = pl.ds(pl.multiple_of(g * GROUP * n_steps, GROUP * n_steps), GROUP * n_steps)
        return pltpu.make_async_copy(ostage.at[rows], o_ref.at[rows], o_sem.at[g])

    def start_in(g, c):
        cache_in(g, 0).start()
        cache_in(g, 1).start()
        return c

    lax.fori_loop(0, n_groups, start_in, 0)

    ri = lax.broadcasted_iota(jnp.int32, (qrows, rows_kv), 0)
    ci = lax.broadcasted_iota(jnp.int32, (qrows, rows_kv), 1)
    row_kv = ri // (qrows // kv)
    thr[...] = jnp.where(ci % kv == row_kv, ci - kv * (ri % n_steps), 1 << 24)

    hid_cp.wait()
    gain = norm_ref[...].astype(F32)
    chunk = 32

    def norm_rows(i, c):
        rows = pl.ds(pl.multiple_of(i * chunk, chunk), chunk)
        x = hid[rows, :].astype(F32)
        inv = lax.rsqrt(jnp.mean(x * x, axis=-1, keepdims=True) + NORM_EPS)
        normed[rows, :] = (x * inv * gain).astype(BF16)
        return c

    lax.fori_loop(0, n_rows // chunk, norm_rows, 0)

    pi = lax.broadcasted_iota(jnp.int32, (n_rows, n_rows), 0)
    pj = lax.broadcasted_iota(jnp.int32, (n_rows, n_rows), 1)
    perm = jnp.where(pj == (pi % n_steps) * n_batch + pi // n_steps, 1.0, 0.0).astype(BF16)

    def norm_rope(x, g):
        inv = lax.rsqrt(jnp.mean(x * x, axis=-1, keepdims=True) + NORM_EPS)
        x = x * inv * g
        return x * cos_ref[...] + pltpu.roll(x, hd // 2, 1) * sin_ref[...]

    qg = qg_ref[...].astype(F32)
    kg = kg_ref[...].astype(F32)
    for i in range(n_q + 2):
        w_cps[i].wait()
        if i < n_q:
            raw = dot(normed[...], wq[:, i * 256:(i + 1) * 256])
        elif i == n_q:
            raw = dot(normed[...], wk[...])
        else:
            raw = dot(normed[...], wv[...])
        if i <= n_q:
            g = qg if i < n_q else kg
            raw = jnp.concatenate([norm_rope(raw[:, :hd], g), norm_rope(raw[:, hd:], g)], axis=1)
        done = dot(perm, raw.astype(BF16))
        if i < n_q:
            qs[:, i * 256:(i + 1) * 256] = done
        elif i == n_q:
            ks[...] = done
        else:
            vs[...] = done

    scale = hd ** -0.5
    grows = GROUP * n_steps
    lane = lax.broadcasted_iota(jnp.int32, (grows, STATS), 1)
    win_rows = lax.broadcasted_iota(jnp.int32, (32, hd), 0)

    def group_step(g, c):
        cache_in(g, 0).wait()
        cache_in(g, 1).wait()
        rows = pl.ds(pl.multiple_of(g * grows, grows), grows)
        q_slab = qs[rows, :]
        k_slab = ks[rows, :]
        v_slab = vs[rows, :]
        outs, maxes, sums = [], [], []
        for r in range(GROUP):
            b = g * GROUP + r
            off = kv * (start_ref[b] - blk_start)
            win = pl.multiple_of(jnp.clip((off // 16) * 16, 0, rows_kv - 32), 16)
            for buf, slab in ((kbuf, k_slab), (vbuf, v_slab)):
                cur = buf[b, pl.ds(win, 32), :].astype(F32)
                for j in range(n_steps):
                    for h in range(kv):
                        new = slab[r * n_steps + j:r * n_steps + j + 1, h * hd:(h + 1) * hd]
                        cur = jnp.where(win_rows == off + kv * j + h - win, new, cur)
                buf[b, pl.ds(win, 32), :] = cur.astype(BF16)
            q = jnp.concatenate([q_slab[r * n_steps:(r + 1) * n_steps, h * hd:(h + 1) * hd] for h in range(heads)], axis=0)
            s = lax.dot_general(q.astype(BF16), kbuf[b], (((1,), (1,)), ((), ())), preferred_element_type=F32) * scale
            keep = thr[...] <= off + kv - 1
            s = jnp.where(keep, s, NEG)
            m = jnp.max(s, axis=-1, keepdims=True)
            p = jnp.where(keep, jnp.exp(s - m), 0.0)
            sums.append(jnp.sum(p, axis=-1, keepdims=True))
            maxes.append(m)
            outs.append(dot(p.astype(BF16), vbuf[b]))
        stats = jnp.zeros((grows, STATS), F32)
        for h in range(heads):
            sl = slice(h * n_steps, (h + 1) * n_steps)
            ostage[rows, h * hd:(h + 1) * hd] = jnp.concatenate([o[sl] for o in outs], axis=0)
            stats = jnp.where(lane == h, jnp.concatenate([m[sl] for m in maxes], axis=0), stats)
            stats = jnp.where(lane == heads + h, jnp.concatenate([t[sl] for t in sums], axis=0), stats)
        ostage[rows, heads * hd:] = stats
        cache_out(g, 0).start()
        cache_out(g, 1).start()
        o_out(g).start()
        return c

    lax.fori_loop(0, n_groups, group_step, 0)

    def drain(g, c):
        cache_out(g, 0).wait()
        cache_out(g, 1).wait()
        o_out(g).wait()
        return c

    lax.fori_loop(0, n_groups, drain, 0)


def attention(start_pos, hidden, cos, sin, attn_norm, q_gain, k_gain, w_q, w_k, w_v, k_cache, v_cache):
    n_rows, d_model = hidden.shape
    n_batch, rows_kv, hd = k_cache.shape
    heads = w_q.shape[1] // hd
    n_groups = n_batch // GROUP
    n_steps = n_rows // n_batch
    n_w = w_q.shape[1] // 256 + 2
    width = heads * hd + STATS
    vmem = pl.BlockSpec(memory_space=pltpu.VMEM)
    hbm = pl.BlockSpec(memory_space=pl.ANY)
    return pl.pallas_call(
        attn_kernel,
        out_shape=(jax.ShapeDtypeStruct((n_rows, width), F32),
                   jax.ShapeDtypeStruct(k_cache.shape, BF16), jax.ShapeDtypeStruct(v_cache.shape, BF16)),
        in_specs=[pl.BlockSpec(memory_space=pltpu.SMEM), hbm, vmem, vmem, vmem, vmem, vmem, hbm, hbm, hbm, hbm, hbm],
        out_specs=(hbm, hbm, hbm),
        scratch_shapes=[
            pltpu.VMEM((n_rows, d_model), BF16), pltpu.VMEM((n_rows, d_model), BF16),
            pltpu.VMEM(w_q.shape, BF16), pltpu.VMEM(w_k.shape, BF16), pltpu.VMEM(w_v.shape, BF16),
            pltpu.VMEM(k_cache.shape, BF16), pltpu.VMEM(v_cache.shape, BF16),
            pltpu.VMEM((n_rows, w_q.shape[1]), F32), pltpu.VMEM((n_rows, w_k.shape[1]), F32),
            pltpu.VMEM((n_rows, w_v.shape[1]), F32), pltpu.VMEM((n_rows, width), F32),
            pltpu.VMEM((heads * n_steps, rows_kv), jnp.int32),
            pltpu.SemaphoreType.DMA, pltpu.SemaphoreType.DMA((n_w,)),
            pltpu.SemaphoreType.DMA((2, n_groups)), pltpu.SemaphoreType.DMA((2, n_groups)),
            pltpu.SemaphoreType.DMA((n_groups,)),
        ],
        compiler_params=pltpu.CompilerParams(vmem_limit_bytes=60_000_000),
        name="attn",
    )(start_pos, hidden, cos, sin, attn_norm, q_gain, k_gain, w_q, w_k, w_v, k_cache, v_cache)


def mlp_kernel(o_ref, hid_ref, norm_ref, wo_ref, wg_ref, wu_ref, wd_ref,
               out_ref,
               x, wo, wg, wu, wd, loc, dbuf, ysend, yrecv, attn, pbuf, in_leaf, in_mid, tbuf, rbuf, mlp_in, act, fbuf, fy, fd,
               x_sem, w_sem, l_sem, d_ssem, d_rsem, y_ssem, y_rsem,
               up_s, up_r, mid_s, mid_r, dn_s, dn_r, fy_s, fy_r, fd_s, fd_r):
    me = lax.axis_index('sp')
    tp = lax.axis_index('tp')
    core = me % 2
    mate = me + 1 - 2 * core
    oth = (me + 2) % 4
    mate_oth = (mate + 2) % 4
    side = tp + 1 - 2 * (tp % 2)
    mid = 3 - tp
    inner = jnp.logical_or(tp == 1, tp == 2)
    leaf = jnp.logical_or(tp == 0, tp == 3)

    n_pieces, n_rows, _ = rbuf.shape
    width = loc.shape[2]
    hd = 128
    heads = (width - STATS) // hd
    n_chunks = dbuf.shape[1]
    crows = dbuf.shape[2]
    n_steps = out_ref.shape[0]
    n_req = n_rows // n_steps

    w_cps = [pltpu.make_async_copy(s, d, w_sem.at[i]) for i, (s, d) in
             enumerate(((wo_ref, wo), (wg_ref, wg), (wu_ref, wu), (wd_ref, wd)))]
    l_cps = [pltpu.make_async_copy(o_ref.at[oth], loc.at[0], l_sem.at[0]),
             pltpu.make_async_copy(o_ref.at[me], loc.at[1], l_sem.at[1])]
    x_cps = [pltpu.make_async_copy(hid_ref.at[i, pl.ds(pl.multiple_of(me * n_req, n_req), n_req), :],
                                   x.at[pl.ds(i * n_req, n_req), :], x_sem.at[i]) for i in range(n_steps)]
    for cp in l_cps:
        cp.start()
    w_cps[0].start()
    for cp in x_cps:
        cp.start()
    for cp in w_cps[1:]:
        cp.start()

    barrier = pltpu.get_barrier_semaphore()
    for dev in ({'sp': mate}, {'sp': oth}, {'tp': side}):
        pl.semaphore_signal(barrier, inc=1, device_id=dev, device_id_type=MESH)

    @pl.when(inner)
    def _():
        pl.semaphore_signal(barrier, inc=1, device_id={'tp': mid}, device_id_type=MESH)
        pl.semaphore_wait(barrier, 4)

    @pl.when(leaf)
    def _():
        pl.semaphore_wait(barrier, 3)

    def remote(src, dst, ssem, rsem, dev):
        return pltpu.make_async_remote_copy(src_ref=src, dst_ref=dst, send_sem=ssem, recv_sem=rsem,
                                            device_id=dev, device_id_type=MESH)

    def d_copy(which, i):
        blk = (mate_oth, mate)[which]
        return remote(o_ref.at[blk, pl.ds(i * crows, crows), :], dbuf.at[which, i], d_ssem.at[which, i], d_rsem.at[which, i],
                      {'sp': mate})

    def y_copy(i):
        return remote(ysend.at[i], yrecv.at[i], y_ssem.at[i], y_rsem.at[i], {'sp': oth})

    for which in range(2):
        for i in range(n_chunks):
            d_copy(which, i).start()

    aw = heads * hd

    def weights(sa, sb):
        m = jnp.maximum(sa, sb)
        ea = jnp.exp(sa - m)
        eb = jnp.exp(sb - m)
        tot = ea * pltpu.roll(sa, STATS - heads, 1) + eb * pltpu.roll(sb, STATS - heads, 1)
        return m, ea, eb, tot

    def pack_stats(m, tot):
        lane = lax.broadcasted_iota(jnp.int32, m.shape, 1)
        return jnp.where(lane < heads, m, pltpu.roll(tot, heads, 1))

    def merge(a, ai, b, bi, dst, di):
        m, ea, eb, tot = weights(a[ai + (slice(aw, None),)], b[bi + (slice(aw, None),)])
        for h in range(heads):
            sl = (slice(h * hd, (h + 1) * hd),)
            dst[di + sl] = a[ai + sl] * ea[:, h:h + 1] + b[bi + sl] * eb[:, h:h + 1]
        dst[di + (slice(aw, None),)] = pack_stats(m, tot)

    l_cps[0].wait()
    for i in range(n_chunks):
        d_copy(0, i).wait_recv()
        rs = slice(i * crows, (i + 1) * crows)
        merge(loc, (0, rs), dbuf, (0, i, slice(None)), ysend, (i, slice(None)))
        y_copy(i).start()
    l_cps[1].wait()
    for i in range(n_chunks):
        d_copy(1, i).wait_recv()
        rs = slice(i * crows, (i + 1) * crows)
        merge(loc, (1, rs), dbuf, (1, i, slice(None)), loc, (1, rs))
    for i in range(n_chunks):
        y_copy(i).wait_recv()
        rs = slice(i * crows, (i + 1) * crows)
        m, ea, eb, tot = weights(loc[1, rs, aw:], yrecv[i, :, aw:])
        for h in range(heads):
            sl = slice(h * hd, (h + 1) * hd)
            val = loc[1, rs, sl] * ea[:, h:h + 1] + yrecv[i, :, sl] * eb[:, h:h + 1]
            attn[rs, sl] = (val / tot[:, h:h + 1]).astype(BF16)

    pi = lax.broadcasted_iota(jnp.int32, (n_rows, n_rows), 0)
    pj = lax.broadcasted_iota(jnp.int32, (n_rows, n_rows), 1)
    perm = jnp.where(pj == (pi % n_req) * n_steps + pi // n_req, 1.0, 0.0).astype(BF16)
    attn[...] = dot(perm, attn[...]).astype(BF16)

    def up(a, k):
        return remote(pbuf.at[a, k], in_leaf.at[a, k], up_s.at[a, k], up_r.at[a, k], {'tp': side})

    def across(a, k):
        return remote(pbuf.at[a, k], in_mid.at[a, k], mid_s.at[a, k], mid_r.at[a, k], {'tp': mid})

    def down(a, k):
        return remote(tbuf.at[a, k], tbuf.at[a, k], dn_s.at[a, k], dn_r.at[a, k], {'tp': side})

    def all_reduce(a, part, finish):
        @pl.when(leaf)
        def _():
            def send(k, c):
                pbuf[a, k] = part(k)
                up(a, k).start()
                return c
            lax.fori_loop(0, n_pieces, send, 0)

            def take(k, c):
                down(a, k).wait_recv()
                finish(k)
                return c
            lax.fori_loop(0, n_pieces, take, 0)

        @pl.when(inner)
        def _():
            def stage_a(k):
                mine = part(k)
                up(a, k).wait_recv()
                pbuf[a, k] = mine + in_leaf[a, k]
                across(a, k).start()

            def stage_b(k):
                across(a, k).wait_recv()
                tbuf[a, k] = pbuf[a, k] + in_mid[a, k]
                down(a, k).start()
                finish(k)

            for k in range(LAG):
                stage_a(k)

            def body(k, c):
                stage_a(k)
                stage_b(k - LAG)
                return c
            lax.fori_loop(LAG, n_pieces, body, 0)
            for k in range(n_pieces - LAG, n_pieces):
                stage_b(k)

    def cols(k):
        return pl.ds(pl.multiple_of(k * PIECE, PIECE), PIECE)

    w_cps[0].wait()
    for cp in x_cps:
        cp.wait()

    def take_r(k):
        r = (x[:, cols(k)].astype(F32) + tbuf[0, k]).astype(BF16).astype(F32)
        rbuf[k] = r

    all_reduce(0, lambda k: dot(attn[...], wo[:, cols(k)]), take_r)

    sq = jnp.zeros((n_rows, 128), F32)
    for k in range(n_pieces):
        r = rbuf[k]
        for j in range(PIECE // 128):
            piece = r[:, j * 128:(j + 1) * 128]
            sq = sq + piece * piece
    d_model = n_pieces * PIECE
    inv = lax.rsqrt(jnp.sum(sq, axis=-1, keepdims=True) * (1.0 / d_model) + NORM_EPS)
    for k in range(n_pieces):
        g = norm_ref[:, k * PIECE:(k + 1) * PIECE].astype(F32)
        mlp_in[:, k * PIECE:(k + 1) * PIECE] = (rbuf[k] * inv * g).astype(BF16)

    w_cps[1].wait()
    w_cps[2].wait()
    ffn = wg.shape[1]
    wide = 256

    def gate_up(sl):
        gate = dot(mlp_in[...], wg[:, sl])
        upv = dot(mlp_in[...], wu[:, sl])
        act[:, sl] = (gate * (1.0 / (1.0 + jnp.exp(-gate))) * upv).astype(BF16)

    def gu_body(j, c):
        gate_up(pl.ds(pl.multiple_of(j * wide, wide), wide))
        return c
    lax.fori_loop(0, ffn // wide, gu_body, 0)
    if ffn % wide:
        gate_up(pl.ds(ffn // wide * wide, ffn % wide))

    w_cps[3].wait()

    def put(blk, k, val):
        val = val.astype(BF16)
        for i in range(n_steps):
            out_ref[i, pl.ds(pl.multiple_of(blk * n_req, n_req), n_req), cols(k)] = val[i * n_req:(i + 1) * n_req]

    def f_y(k):
        return remote(fbuf.at[k], fy.at[k], fy_s.at[k], fy_r.at[k], {'sp': oth})

    def f_d(which, k):
        src = (fbuf, fy)[which]
        return remote(src.at[k], fd.at[which, k], fd_s.at[which, k], fd_r.at[which, k], {'sp': mate})

    def forward(k):
        f_y(k).wait_recv()
        f_d(1, k).start()
        put(oth, k, fy[k])

    def finish_out(k):
        val = (rbuf[k] + tbuf[1, k]).astype(BF16)
        fbuf[k] = val.astype(F32)
        f_y(k).start()
        f_d(0, k).start()
        put(me, k, val)

        if isinstance(k, int):
            if k >= LAG:
                forward(k - LAG)
        else:
            @pl.when(k >= LAG)
            def _():
                forward(k - LAG)

    all_reduce(1, lambda k: dot(act[...], wd[:, cols(k)]), finish_out)
    for k in range(n_pieces - LAG, n_pieces):
        forward(k)

    def last(k, c):
        f_d(0, k).wait_recv()
        put(mate, k, fd[0, k])
        f_d(1, k).wait_recv()
        put(mate_oth, k, fd[1, k])
        return c
    lax.fori_loop(0, n_pieces, last, 0)

    for which in range(2):
        for i in range(n_chunks):
            d_copy(which, i).wait_send()
    for i in range(n_chunks):
        y_copy(i).wait_send()

    def sends(k, c):
        f_y(k).wait_send()
        f_d(0, k).wait_send()
        f_d(1, k).wait_send()
        for a in range(2):
            @pl.when(leaf)
            def _():
                up(a, k).wait_send()

            @pl.when(inner)
            def _():
                across(a, k).wait_send()
                down(a, k).wait_send()
        return c
    lax.fori_loop(0, n_pieces, sends, 0)


def mlp(o_part, hidden, mlp_norm, w_o, w_gate, w_up, w_down):
    n_blk, n_rows, width = o_part.shape
    n_steps, n_batch, d_model = hidden.shape
    n_pieces = d_model // PIECE
    n_chunks = 4
    crows = n_rows // n_chunks
    ffn = w_gate.shape[1]
    vmem = pl.BlockSpec(memory_space=pltpu.VMEM)
    hbm = pl.BlockSpec(memory_space=pl.ANY)
    dma = pltpu.SemaphoreType.DMA
    piece = (n_pieces, n_rows, PIECE)
    return pl.pallas_call(
        mlp_kernel,
        out_shape=jax.ShapeDtypeStruct(hidden.shape, BF16),
        in_specs=[hbm, hbm, vmem, hbm, hbm, hbm, hbm],
        out_specs=vmem,
        scratch_shapes=[
            pltpu.VMEM((n_rows, d_model), BF16),
            pltpu.VMEM(w_o.shape, BF16), pltpu.VMEM(w_gate.shape, BF16),
            pltpu.VMEM(w_up.shape, BF16), pltpu.VMEM(w_down.shape, BF16),
            pltpu.VMEM((2, n_rows, width), F32), pltpu.VMEM((2, n_chunks, crows, width), F32),
            pltpu.VMEM((n_chunks, crows, width), F32), pltpu.VMEM((n_chunks, crows, width), F32),
            pltpu.VMEM((n_rows, w_o.shape[0]), BF16),
            pltpu.VMEM((2,) + piece, F32), pltpu.VMEM((2,) + piece, F32),
            pltpu.VMEM((2,) + piece, F32), pltpu.VMEM((2,) + piece, F32),
            pltpu.VMEM(piece, F32), pltpu.VMEM((n_rows, d_model), BF16), pltpu.VMEM((n_rows, ffn), BF16),
            pltpu.VMEM(piece, F32), pltpu.VMEM(piece, F32), pltpu.VMEM((2,) + piece, F32),
            dma((n_steps,)), dma((4,)), dma((2,)),
            dma((2, n_chunks)), dma((2, n_chunks)), dma((n_chunks,)), dma((n_chunks,)),
            dma((2, n_pieces)), dma((2, n_pieces)), dma((2, n_pieces)), dma((2, n_pieces)),
            dma((2, n_pieces)), dma((2, n_pieces)),
            dma((n_pieces,)), dma((n_pieces,)), dma((2, n_pieces)), dma((2, n_pieces)),
        ],
        compiler_params=pltpu.CompilerParams(vmem_limit_bytes=VMEM_LIMIT, collective_id=0, has_side_effects=True),
        name="combine_mlp",
    )(o_part, hidden, mlp_norm, w_o, w_gate, w_up, w_down)


def solution(mesh):
    cache_spec = P('dp', 'sp', 'tp', None)
    col_spec = P(None, 'tp')
    row_spec = P('tp', None)
    in_specs = (P(None, 'dp', None), P('dp'), cache_spec, cache_spec, col_spec, col_spec, col_spec, row_spec,
                col_spec, col_spec, row_spec, P(), P(), P(), P())
    out_specs = (P(None, 'dp', None), cache_spec, cache_spec)

    def shard_body(hidden, start_pos, k_cache, v_cache, w_q, w_k, w_v, w_o, w_gate, w_up, w_down, attn_norm, mlp_norm, q_gain, k_gain):
        n_steps, n_batch, d_model = hidden.shape
        _, seq, kv, hd = k_cache.shape
        half = hd // 2
        freqs = ROPE_BASE ** (-(jnp.arange(half, dtype=F32) * (2.0 / hd)))
        tok_pos = (start_pos[None, :] + jnp.arange(n_steps)[:, None]).reshape(-1)
        angles = tok_pos.astype(F32)[:, None] * freqs[None, :]
        cos, sin = jnp.cos(angles), jnp.sin(angles)
        cos = jnp.concatenate([cos, cos], axis=1)
        sin = jnp.concatenate([-sin, sin], axis=1)
        o_part, k_out, v_out = attention(
            start_pos, hidden.reshape(-1, d_model), cos, sin, attn_norm[None], q_gain[None], k_gain[None],
            w_q, w_k, w_v, k_cache.reshape(n_batch, seq * kv, hd), v_cache.reshape(n_batch, seq * kv, hd))
        n_sp = 4
        out = mlp(o_part.reshape(n_sp, -1, o_part.shape[1]), hidden, mlp_norm[None], w_o, w_gate, w_up, w_down)
        return out, k_out.reshape(k_cache.shape), v_out.reshape(v_cache.shape)

    return jax.shard_map(shard_body, mesh=mesh, in_specs=in_specs, out_specs=out_specs, check_vma=False)
```

```python
import functools
import jax
import jax.numpy as jnp
import numpy as np
from jax import lax
from jax.experimental import pallas as pl
from jax.experimental.pallas import tpu as pltpu
from jax.sharding import PartitionSpec as P

ROPE_BASE = 1000000.0
NORM_EPS = 1e-06
NEG = -3.0e38
F32 = jnp.float32
BF16 = jnp.bfloat16
MESH = pl.DeviceIdType.MESH
STATS = 128
GROUP = 8
PIECE = 256
LAG = 3
VMEM_LIMIT = 66_900_000


def dot(a, b):
    return jnp.dot(a, b, preferred_element_type=F32)


def attn_kernel(start_ref, hid_ref, freq_ref, norm_ref, qg_ref, kg_ref, wq_ref, wk_ref, wv_ref, kc_ref, vc_ref,
                o_ref, ko_ref, vo_ref,
                hid, normed, wq, wk, wv, kbuf, vbuf, cos, sin, raw, qs, ks, vs, ostage, thr, gain,
                hid_sem, w_sem, in_sem, out_sem, o_sem):
    n_rows, d_model = hid.shape
    n_batch, rows_kv, hd = kbuf.shape
    n_steps = n_rows // n_batch
    heads = wq.shape[1] // hd
    kv = wk.shape[1] // hd
    seq = rows_kv // kv
    n_groups = n_batch // GROUP
    qrows = heads * n_steps
    blk_start = lax.axis_index('sp') * seq

    hid_cp = pltpu.make_async_copy(hid_ref, hid, hid_sem)
    hid_cp.start()
    n_q = wq.shape[1] // 256
    w_cps = []
    for i in range(n_q):
        w_cps.append(pltpu.make_async_copy(wq_ref.at[:, pl.ds(i * 256, 256)], wq.at[:, pl.ds(i * 256, 256)], w_sem.at[i]))
    w_cps.append(pltpu.make_async_copy(wk_ref, wk, w_sem.at[n_q]))
    w_cps.append(pltpu.make_async_copy(wv_ref, wv, w_sem.at[n_q + 1]))
    for cp in w_cps:
        cp.start()

    def cache_in(g, which):
        src, dst = ((kc_ref, kbuf), (vc_ref, vbuf))[which]
        rows = pl.ds(g * GROUP, GROUP)
        return pltpu.make_async_copy(src.at[rows], dst.at[rows], in_sem.at[which, g])

    def cache_out(g, which):
        src, dst = ((kbuf, ko_ref), (vbuf, vo_ref))[which]
        rows = pl.ds(g * GROUP, GROUP)
        return pltpu.make_async_copy(src.at[rows], dst.at[rows], out_sem.at[which, g])

    def o_out(g):
        rows = pl.ds(pl.multiple_of(g * GROUP * n_steps, GROUP * n_steps), GROUP * n_steps)
        return pltpu.make_async_copy(ostage.at[rows], o_ref.at[rows], o_sem.at[g])

    def start_in(g, c):
        cache_in(g, 0).start()
        cache_in(g, 1).start()
        return c

    lax.fori_loop(0, n_groups, start_in, 0)

    ri = lax.broadcasted_iota(jnp.int32, (qrows, rows_kv), 0)
    ci = lax.broadcasted_iota(jnp.int32, (qrows, rows_kv), 1)
    row_kv = ri // (qrows // kv)
    thr[...] = jnp.where(ci % kv == row_kv, ci - kv * (ri % n_steps), 1 << 24)

    def set_pos(b, c):
        for i in range(n_steps):
            cos[pl.ds(b * n_steps + i, 1), :] = jnp.full((1, hd), start_ref[b] + i, jnp.int32).astype(F32)
        return c

    lax.fori_loop(0, n_batch, set_pos, 0)
    trows = 64
    low = lax.broadcasted_iota(jnp.int32, (trows, hd), 1) < hd // 2

    def table(i, c):
        rows = pl.ds(pl.multiple_of(i * trows, trows), trows)
        angle = cos[rows, :] * freq_ref[...]
        s = jnp.sin(angle)
        sin[rows, :] = jnp.where(low, -s, s)
        cos[rows, :] = jnp.cos(angle)
        return c

    lax.fori_loop(0, n_rows // trows, table, 0)

    for j in range(d_model // 128):
        gain[:, j * 128:(j + 1) * 128] = jnp.broadcast_to(norm_ref[j:j + 1, :].astype(F32), (8, 128))

    hid_cp.wait()
    chunk = 16

    def norm_rows(i, c):
        for u in range(4):
            rows = pl.ds(pl.multiple_of(i * 4 * chunk + u * chunk, chunk), chunk)
            x = hid[rows, :].astype(F32)
            inv = lax.rsqrt(jnp.mean(x * x, axis=-1, keepdims=True) + NORM_EPS)
            x = x * inv
            normed[rows, :] = jnp.concatenate([x[:8] * gain[...], x[8:] * gain[...]], axis=0).astype(BF16)
        return c

    lax.fori_loop(0, n_rows // (4 * chunk), norm_rows, 0)

    pi = lax.broadcasted_iota(jnp.int32, (n_rows, n_rows), 0)
    pj = lax.broadcasted_iota(jnp.int32, (n_rows, n_rows), 1)
    perm = jnp.where(pj == (pi % n_steps) * n_batch + pi // n_steps, 1.0, 0.0).astype(BF16)
    for j in range(d_model // 256):
        sl = slice(j * 256, (j + 1) * 256)
        hid[:, sl] = dot(perm, normed[:, sl]).astype(BF16)

    def norm_rope(x, g, rows):
        inv = lax.rsqrt(jnp.mean(x * x, axis=-1, keepdims=True) + NORM_EPS)
        x = x * inv * g
        return (x * cos[rows, :] + pltpu.roll(x, hd // 2, 1) * sin[rows, :]).astype(BF16).astype(F32)

    qg = qg_ref[...].astype(F32)
    kg = kg_ref[...].astype(F32)

    def post(i):
        for r in range(n_rows // 64):
            rows = slice(r * 64, (r + 1) * 64)
            for h in range(2):
                x = raw[i % 2, rows, h * hd:(h + 1) * hd]
                if i < n_q:
                    qs[rows, i * 256 + h * hd:i * 256 + (h + 1) * hd] = norm_rope(x, qg, rows)
                elif i == n_q:
                    ks[rows, h * hd:(h + 1) * hd] = norm_rope(x, kg, rows)
                else:
                    vs[rows, h * hd:(h + 1) * hd] = x.astype(BF16).astype(F32)

    for i in range(n_q + 3):
        if i < n_q + 2:
            w_cps[i].wait()
            w = wq[:, i * 256:(i + 1) * 256] if i < n_q else (wk[...] if i == n_q else wv[...])
            raw[i % 2] = dot(hid[...], w)
        if i > 0:
            post(i - 1)

    scale = hd ** -0.5
    grows = GROUP * n_steps
    lane = lax.broadcasted_iota(jnp.int32, (grows, STATS), 1)
    win_rows = lax.broadcasted_iota(jnp.int32, (32, hd), 0)

    def group_step(g, c):
        cache_in(g, 0).wait()
        cache_in(g, 1).wait()
        rows = pl.ds(pl.multiple_of(g * grows, grows), grows)
        q_slab = qs[rows, :]
        offs = []
        for r in range(GROUP):
            b = g * GROUP + r
            off = kv * (start_ref[b] - blk_start)
            offs.append(off)
            win = pl.multiple_of(jnp.clip((off // 16) * 16, 0, rows_kv - 32), 16)
            for buf, new_ref in ((kbuf, ks), (vbuf, vs)):
                slab = new_ref[rows, :]
                cur = buf[b, pl.ds(win, 32), :].astype(F32)
                for j in range(n_steps):
                    for h in range(kv):
                        new = slab[r * n_steps + j:r * n_steps + j + 1, h * hd:(h + 1) * hd]
                        cur = jnp.where(win_rows == off + kv * j + h - win, new, cur)
                buf[b, pl.ds(win, 32), :] = cur.astype(BF16)
        scores = []
        for r in range(GROUP):
            q = jnp.concatenate([q_slab[r * n_steps:(r + 1) * n_steps, h * hd:(h + 1) * hd] for h in range(heads)], axis=0)
            scores.append(lax.dot_general(q.astype(BF16), kbuf[g * GROUP + r], (((1,), (1,)), ((), ())),
                                          preferred_element_type=F32))
        probs, maxes, sums = [], [], []
        for r in range(GROUP):
            keep = thr[...] <= offs[r] + kv - 1
            s = jnp.where(keep, scores[r] * scale, NEG)
            m = jnp.max(s, axis=-1, keepdims=True)
            p = jnp.where(keep, jnp.exp(s - m), 0.0)
            sums.append(jnp.sum(p, axis=-1, keepdims=True))
            maxes.append(m)
            probs.append(p.astype(BF16))
        outs = [dot(probs[r], vbuf[g * GROUP + r]) for r in range(GROUP)]
        stats = jnp.zeros((grows, STATS), F32)
        for h in range(heads):
            sl = slice(h * n_steps, (h + 1) * n_steps)
            ostage[rows, h * hd:(h + 1) * hd] = jnp.concatenate([o[sl] for o in outs], axis=0)
            stats = jnp.where(lane == h, jnp.concatenate([m[sl] for m in maxes], axis=0), stats)
            stats = jnp.where(lane == heads + h, jnp.concatenate([t[sl] for t in sums], axis=0), stats)
        ostage[rows, heads * hd:] = stats
        cache_out(g, 0).start()
        cache_out(g, 1).start()
        o_out(g).start()
        return c

    lax.fori_loop(0, n_groups, group_step, 0)

    def drain(g, c):
        cache_out(g, 0).wait()
        cache_out(g, 1).wait()
        o_out(g).wait()
        return c

    lax.fori_loop(0, n_groups, drain, 0)


def attention(start_pos, hidden, freq, attn_norm, q_gain, k_gain, w_q, w_k, w_v, k_cache, v_cache):
    n_rows, d_model = hidden.shape
    n_batch, rows_kv, hd = k_cache.shape
    heads = w_q.shape[1] // hd
    n_groups = n_batch // GROUP
    n_steps = n_rows // n_batch
    n_w = w_q.shape[1] // 256 + 2
    width = heads * hd + STATS
    vmem = pl.BlockSpec(memory_space=pltpu.VMEM)
    hbm = pl.BlockSpec(memory_space=pl.ANY)
    return pl.pallas_call(
        attn_kernel,
        out_shape=(jax.ShapeDtypeStruct((n_rows, width), F32),
                   jax.ShapeDtypeStruct(k_cache.shape, BF16), jax.ShapeDtypeStruct(v_cache.shape, BF16)),
        in_specs=[pl.BlockSpec(memory_space=pltpu.SMEM), hbm, vmem, vmem, vmem, vmem, hbm, hbm, hbm, hbm, hbm],
        out_specs=(hbm, hbm, hbm),
        scratch_shapes=[
            pltpu.VMEM((n_rows, d_model), BF16), pltpu.VMEM((n_rows, d_model), BF16),
            pltpu.VMEM(w_q.shape, BF16), pltpu.VMEM(w_k.shape, BF16), pltpu.VMEM(w_v.shape, BF16),
            pltpu.VMEM(k_cache.shape, BF16), pltpu.VMEM(v_cache.shape, BF16),
            pltpu.VMEM((n_rows, hd), F32), pltpu.VMEM((n_rows, hd), F32), pltpu.VMEM((2, n_rows, 256), F32),
            pltpu.VMEM((n_rows, w_q.shape[1]), F32), pltpu.VMEM((n_rows, w_k.shape[1]), F32),
            pltpu.VMEM((n_rows, w_v.shape[1]), F32), pltpu.VMEM((n_rows, width), F32),
            pltpu.VMEM((heads * n_steps, rows_kv), jnp.int32), pltpu.VMEM((8, d_model), F32),
            pltpu.SemaphoreType.DMA, pltpu.SemaphoreType.DMA((n_w,)),
            pltpu.SemaphoreType.DMA((2, n_groups)), pltpu.SemaphoreType.DMA((2, n_groups)),
            pltpu.SemaphoreType.DMA((n_groups,)),
        ],
        compiler_params=pltpu.CompilerParams(vmem_limit_bytes=60_000_000),
        name="attn",
    )(start_pos, hidden, freq, attn_norm, q_gain, k_gain, w_q, w_k, w_v, k_cache, v_cache)


def mlp_kernel(o_ref, hid_ref, norm_ref, wo_ref, wg_ref, wu_ref, wd_ref,
               out_ref,
               x, wo, wg, wu, wd, loc, dbuf, ysend, yrecv, attn, pbuf, in_leaf, in_mid, tbuf, rbuf, mlp_in, act, fbuf, fy, fd,
               x_sem, w_sem, l_sem, d_ssem, d_rsem, y_ssem, y_rsem,
               up_s, up_r, mid_s, mid_r, dn_s, dn_r, fy_s, fy_r, fd_s, fd_r):
    me = lax.axis_index('sp')
    tp = lax.axis_index('tp')
    core = me % 2
    mate = me + 1 - 2 * core
    oth = (me + 2) % 4
    mate_oth = (mate + 2) % 4
    side = tp + 1 - 2 * (tp % 2)
    mid = 3 - tp
    inner = jnp.logical_or(tp == 1, tp == 2)
    leaf = jnp.logical_or(tp == 0, tp == 3)

    n_pieces, n_rows, _ = rbuf.shape
    width = loc.shape[2]
    hd = 128
    heads = (width - STATS) // hd
    n_chunks = dbuf.shape[1]
    crows = dbuf.shape[2]
    n_steps = out_ref.shape[0]
    n_req = n_rows // n_steps

    w_cps = [pltpu.make_async_copy(s, d, w_sem.at[i]) for i, (s, d) in
             enumerate(((wo_ref, wo), (wg_ref, wg), (wu_ref, wu), (wd_ref, wd)))]
    l_cps = [pltpu.make_async_copy(o_ref.at[oth], loc.at[0], l_sem.at[0]),
             pltpu.make_async_copy(o_ref.at[me], loc.at[1], l_sem.at[1])]
    x_cps = [pltpu.make_async_copy(hid_ref.at[i, pl.ds(pl.multiple_of(me * n_req, n_req), n_req), :],
                                   x.at[pl.ds(i * n_req, n_req), :], x_sem.at[i]) for i in range(n_steps)]
    for cp in l_cps:
        cp.start()
    w_cps[0].start()
    for cp in x_cps:
        cp.start()
    for cp in w_cps[1:]:
        cp.start()

    barrier = pltpu.get_barrier_semaphore()
    for dev in ({'sp': mate}, {'sp': oth}, {'tp': side}):
        pl.semaphore_signal(barrier, inc=1, device_id=dev, device_id_type=MESH)

    @pl.when(inner)
    def _():
        pl.semaphore_signal(barrier, inc=1, device_id={'tp': mid}, device_id_type=MESH)
        pl.semaphore_wait(barrier, 4)

    @pl.when(leaf)
    def _():
        pl.semaphore_wait(barrier, 3)

    def remote(src, dst, ssem, rsem, dev):
        return pltpu.make_async_remote_copy(src_ref=src, dst_ref=dst, send_sem=ssem, recv_sem=rsem,
                                            device_id=dev, device_id_type=MESH)

    def d_copy(which, i):
        blk = (mate_oth, mate)[which]
        return remote(o_ref.at[blk, pl.ds(i * crows, crows), :], dbuf.at[which, i], d_ssem.at[which, i], d_rsem.at[which, i],
                      {'sp': mate})

    def y_copy(i):
        return remote(ysend.at[i], yrecv.at[i], y_ssem.at[i], y_rsem.at[i], {'sp': oth})

    for which in range(2):
        for i in range(n_chunks):
            d_copy(which, i).start()

    aw = heads * hd

    def weights(sa, sb):
        m = jnp.maximum(sa, sb)
        ea = jnp.exp(sa - m)
        eb = jnp.exp(sb - m)
        tot = ea * pltpu.roll(sa, STATS - heads, 1) + eb * pltpu.roll(sb, STATS - heads, 1)
        return m, ea, eb, tot

    def pack_stats(m, tot):
        lane = lax.broadcasted_iota(jnp.int32, m.shape, 1)
        return jnp.where(lane < heads, m, pltpu.roll(tot, heads, 1))

    def merge(a, ai, b, bi, dst, di):
        m, ea, eb, tot = weights(a[ai + (slice(aw, None),)], b[bi + (slice(aw, None),)])
        for h in range(heads):
            sl = (slice(h * hd, (h + 1) * hd),)
            dst[di + sl] = a[ai + sl] * ea[:, h:h + 1] + b[bi + sl] * eb[:, h:h + 1]
        dst[di + (slice(aw, None),)] = pack_stats(m, tot)

    l_cps[0].wait()
    for i in range(n_chunks):
        d_copy(0, i).wait_recv()
        rs = slice(i * crows, (i + 1) * crows)
        merge(loc, (0, rs), dbuf, (0, i, slice(None)), ysend, (i, slice(None)))
        y_copy(i).start()
    l_cps[1].wait()
    for i in range(n_chunks):
        d_copy(1, i).wait_recv()
        rs = slice(i * crows, (i + 1) * crows)
        merge(loc, (1, rs), dbuf, (1, i, slice(None)), loc, (1, rs))
    for i in range(n_chunks):
        y_copy(i).wait_recv()
        rs = slice(i * crows, (i + 1) * crows)
        m, ea, eb, tot = weights(loc[1, rs, aw:], yrecv[i, :, aw:])
        for h in range(heads):
            sl = slice(h * hd, (h + 1) * hd)
            val = loc[1, rs, sl] * ea[:, h:h + 1] + yrecv[i, :, sl] * eb[:, h:h + 1]
            attn[rs, sl] = (val / tot[:, h:h + 1]).astype(BF16)

    pi = lax.broadcasted_iota(jnp.int32, (n_rows, n_rows), 0)
    pj = lax.broadcasted_iota(jnp.int32, (n_rows, n_rows), 1)
    perm = jnp.where(pj == (pi % n_req) * n_steps + pi // n_req, 1.0, 0.0).astype(BF16)
    attn[...] = dot(perm, attn[...]).astype(BF16)

    def up(a, k):
        return remote(pbuf.at[a, k], in_leaf.at[a, k], up_s.at[a, k], up_r.at[a, k], {'tp': side})

    def across(a, k):
        return remote(pbuf.at[a, k], in_mid.at[a, k], mid_s.at[a, k], mid_r.at[a, k], {'tp': mid})

    def down(a, k):
        return remote(tbuf.at[a, k], tbuf.at[a, k], dn_s.at[a, k], dn_r.at[a, k], {'tp': side})

    def all_reduce(a, part, finish):
        @pl.when(leaf)
        def _():
            def send(k, c):
                pbuf[a, k] = part(k)
                up(a, k).start()
                return c
            lax.fori_loop(0, n_pieces, send, 0)

            def take(k, c):
                down(a, k).wait_recv()
                finish(k)
                return c
            lax.fori_loop(0, n_pieces, take, 0)

        @pl.when(inner)
        def _():
            def stage_a(k):
                mine = part(k)
                up(a, k).wait_recv()
                pbuf[a, k] = mine + in_leaf[a, k]
                across(a, k).start()

            def stage_b(k):
                across(a, k).wait_recv()
                tbuf[a, k] = pbuf[a, k] + in_mid[a, k]
                down(a, k).start()
                finish(k)

            for k in range(LAG):
                stage_a(k)

            def body(k, c):
                stage_a(k)
                stage_b(k - LAG)
                return c
            lax.fori_loop(LAG, n_pieces, body, 0)
            for k in range(n_pieces - LAG, n_pieces):
                stage_b(k)

    def cols(k):
        return pl.ds(pl.multiple_of(k * PIECE, PIECE), PIECE)

    w_cps[0].wait()
    for cp in x_cps:
        cp.wait()

    def take_r(k):
        r = (x[:, cols(k)].astype(F32) + tbuf[0, k]).astype(BF16).astype(F32)
        rbuf[k] = r

    all_reduce(0, lambda k: dot(attn[...], wo[:, cols(k)]), take_r)

    sq = jnp.zeros((n_rows, 128), F32)
    for k in range(n_pieces):
        r = rbuf[k]
        for j in range(PIECE // 128):
            piece = r[:, j * 128:(j + 1) * 128]
            sq = sq + piece * piece
    d_model = n_pieces * PIECE
    inv = lax.rsqrt(jnp.sum(sq, axis=-1, keepdims=True) * (1.0 / d_model) + NORM_EPS)
    for k in range(n_pieces):
        for j in range(PIECE // 128):
            c0 = k * PIECE + j * 128
            g = norm_ref[c0 // 128:c0 // 128 + 1, :].astype(F32)
            mlp_in[:, c0:c0 + 128] = (rbuf[k, :, j * 128:(j + 1) * 128] * inv * g).astype(BF16)

    w_cps[1].wait()
    w_cps[2].wait()
    ffn = wg.shape[1]
    wide = 256

    def gate_up(sl):
        gate = dot(mlp_in[...], wg[:, sl])
        upv = dot(mlp_in[...], wu[:, sl])
        act[:, sl] = (gate * (1.0 / (1.0 + jnp.exp(-gate))) * upv).astype(BF16)

    def gu_body(j, c):
        gate_up(pl.ds(pl.multiple_of(j * wide, wide), wide))
        return c
    lax.fori_loop(0, ffn // wide, gu_body, 0)
    if ffn % wide:
        gate_up(pl.ds(ffn // wide * wide, ffn % wide))

    w_cps[3].wait()

    def put(blk, k, val):
        val = val.astype(BF16)
        for i in range(n_steps):
            out_ref[i, pl.ds(pl.multiple_of(blk * n_req, n_req), n_req), cols(k)] = val[i * n_req:(i + 1) * n_req]

    def f_y(k):
        return remote(fbuf.at[k], fy.at[k], fy_s.at[k], fy_r.at[k], {'sp': oth})

    def f_d(which, k):
        src = (fbuf, fy)[which]
        return remote(src.at[k], fd.at[which, k], fd_s.at[which, k], fd_r.at[which, k], {'sp': mate})

    def forward(k):
        f_y(k).wait_recv()
        f_d(1, k).start()
        put(oth, k, fy[k])

    def finish_out(k):
        val = (rbuf[k] + tbuf[1, k]).astype(BF16)
        fbuf[k] = val.astype(F32)
        f_y(k).start()
        f_d(0, k).start()
        put(me, k, val)

        if isinstance(k, int):
            if k >= LAG:
                forward(k - LAG)
        else:
            @pl.when(k >= LAG)
            def _():
                forward(k - LAG)

    all_reduce(1, lambda k: dot(act[...], wd[:, cols(k)]), finish_out)
    for k in range(n_pieces - LAG, n_pieces):
        forward(k)

    def last(k, c):
        f_d(0, k).wait_recv()
        put(mate, k, fd[0, k])
        f_d(1, k).wait_recv()
        put(mate_oth, k, fd[1, k])
        return c
    lax.fori_loop(0, n_pieces, last, 0)

    for which in range(2):
        for i in range(n_chunks):
            d_copy(which, i).wait_send()
    for i in range(n_chunks):
        y_copy(i).wait_send()

    def sends(k, c):
        f_y(k).wait_send()
        f_d(0, k).wait_send()
        f_d(1, k).wait_send()
        for a in range(2):
            @pl.when(leaf)
            def _():
                up(a, k).wait_send()

            @pl.when(inner)
            def _():
                across(a, k).wait_send()
                down(a, k).wait_send()
        return c
    lax.fori_loop(0, n_pieces, sends, 0)


def mlp(o_part, hidden, mlp_norm, w_o, w_gate, w_up, w_down):
    n_blk, n_rows, width = o_part.shape
    n_steps, n_batch, d_model = hidden.shape
    n_pieces = d_model // PIECE
    n_chunks = 4
    crows = n_rows // n_chunks
    ffn = w_gate.shape[1]
    vmem = pl.BlockSpec(memory_space=pltpu.VMEM)
    hbm = pl.BlockSpec(memory_space=pl.ANY)
    dma = pltpu.SemaphoreType.DMA
    piece = (n_pieces, n_rows, PIECE)
    return pl.pallas_call(
        mlp_kernel,
        out_shape=jax.ShapeDtypeStruct(hidden.shape, BF16),
        in_specs=[hbm, hbm, vmem, hbm, hbm, hbm, hbm],
        out_specs=vmem,
        scratch_shapes=[
            pltpu.VMEM((n_rows, d_model), BF16),
            pltpu.VMEM(w_o.shape, BF16), pltpu.VMEM(w_gate.shape, BF16),
            pltpu.VMEM(w_up.shape, BF16), pltpu.VMEM(w_down.shape, BF16),
            pltpu.VMEM((2, n_rows, width), F32), pltpu.VMEM((2, n_chunks, crows, width), F32),
            pltpu.VMEM((n_chunks, crows, width), F32), pltpu.VMEM((n_chunks, crows, width), F32),
            pltpu.VMEM((n_rows, w_o.shape[0]), BF16),
            pltpu.VMEM((2,) + piece, F32), pltpu.VMEM((2,) + piece, F32),
            pltpu.VMEM((2,) + piece, F32), pltpu.VMEM((2,) + piece, F32),
            pltpu.VMEM(piece, F32), pltpu.VMEM((n_rows, d_model), BF16), pltpu.VMEM((n_rows, ffn), BF16),
            pltpu.VMEM(piece, F32), pltpu.VMEM(piece, F32), pltpu.VMEM((2,) + piece, F32),
            dma((n_steps,)), dma((4,)), dma((2,)),
            dma((2, n_chunks)), dma((2, n_chunks)), dma((n_chunks,)), dma((n_chunks,)),
            dma((2, n_pieces)), dma((2, n_pieces)), dma((2, n_pieces)), dma((2, n_pieces)),
            dma((2, n_pieces)), dma((2, n_pieces)),
            dma((n_pieces,)), dma((n_pieces,)), dma((2, n_pieces)), dma((2, n_pieces)),
        ],
        compiler_params=pltpu.CompilerParams(vmem_limit_bytes=VMEM_LIMIT, collective_id=0, has_side_effects=True),
        name="combine_mlp",
    )(o_part, hidden, mlp_norm, w_o, w_gate, w_up, w_down)


def solution(mesh):
    cache_spec = P('dp', 'sp', 'tp', None)
    col_spec = P(None, 'tp')
    row_spec = P('tp', None)
    in_specs = (P(None, 'dp', None), P('dp'), cache_spec, cache_spec, col_spec, col_spec, col_spec, row_spec,
                col_spec, col_spec, row_spec, P(), P(), P(), P())
    out_specs = (P(None, 'dp', None), cache_spec, cache_spec)

    def shard_body(hidden, start_pos, k_cache, v_cache, w_q, w_k, w_v, w_o, w_gate, w_up, w_down, attn_norm, mlp_norm, q_gain, k_gain):
        n_steps, n_batch, d_model = hidden.shape
        _, seq, kv, hd = k_cache.shape
        half = np.arange(hd // 2)
        freq = ROPE_BASE ** (-half * (2.0 / hd))
        freq = jnp.asarray(np.concatenate([freq, freq])[None], F32)
        o_part, k_out, v_out = attention(
            start_pos, hidden.reshape(-1, d_model), freq, attn_norm.reshape(-1, 128), q_gain[None], k_gain[None],
            w_q, w_k, w_v, k_cache.reshape(n_batch, seq * kv, hd), v_cache.reshape(n_batch, seq * kv, hd))
        n_sp = 4
        out = mlp(o_part.reshape(n_sp, -1, o_part.shape[1]), hidden, mlp_norm.reshape(-1, 128), w_o, w_gate, w_up, w_down)
        return out, k_out.reshape(k_cache.shape), v_out.reshape(v_cache.shape)

    return jax.shard_map(shard_body, mesh=mesh, in_specs=in_specs, out_specs=out_specs, check_vma=False)
```

```python
import functools
import jax
import jax.numpy as jnp
import numpy as np
from jax import lax
from jax.experimental import pallas as pl
from jax.experimental.pallas import tpu as pltpu
from jax.sharding import PartitionSpec as P

ROPE_BASE = 1000000.0
NORM_EPS = 1e-06
NEG = -3.0e38
F32 = jnp.float32
BF16 = jnp.bfloat16
MESH = pl.DeviceIdType.MESH
STATS = 128
GROUP = 8
PIECE = 256
LAG = 5
FLAG = 4
GU_BLOCK = 384
FLUSH = True
VMEM_LIMIT = 66_900_000


def dot(a, b):
    return jnp.dot(a, b, preferred_element_type=F32)


def attn_kernel(start_ref, hid_ref, freq_ref, norm_ref, qg_ref, kg_ref, wq_ref, wk_ref, wv_ref, kc_ref, vc_ref,
                o_ref, ko_ref, vo_ref,
                hid, normed, wq, wk, wv, kbuf, vbuf, cos, sin, raw, qs, ks, vs, ostage, thr, gain,
                hid_sem, w_sem, in_sem, out_sem, o_sem):
    n_rows, d_model = hid.shape
    n_batch, rows_kv, hd = kbuf.shape
    n_steps = n_rows // n_batch
    heads = wq.shape[1] // hd
    kv = wk.shape[1] // hd
    seq = rows_kv // kv
    n_groups = n_batch // GROUP
    qrows = heads * n_steps
    blk_start = lax.axis_index('sp') * seq

    hid_cp = pltpu.make_async_copy(hid_ref, hid, hid_sem)
    hid_cp.start()
    n_q = wq.shape[1] // 256
    w_cps = []
    for i in range(n_q):
        w_cps.append(pltpu.make_async_copy(wq_ref.at[:, pl.ds(i * 256, 256)], wq.at[:, pl.ds(i * 256, 256)], w_sem.at[i]))
    w_cps.append(pltpu.make_async_copy(wk_ref, wk, w_sem.at[n_q]))
    w_cps.append(pltpu.make_async_copy(wv_ref, wv, w_sem.at[n_q + 1]))
    for cp in w_cps:
        cp.start()

    def cache_in(g, which):
        src, dst = ((kc_ref, kbuf), (vc_ref, vbuf))[which]
        rows = pl.ds(g * GROUP, GROUP)
        return pltpu.make_async_copy(src.at[rows], dst.at[rows], in_sem.at[which, g])

    def cache_out(g, which):
        src, dst = ((kbuf, ko_ref), (vbuf, vo_ref))[which]
        rows = pl.ds(g * GROUP, GROUP)
        return pltpu.make_async_copy(src.at[rows], dst.at[rows], out_sem.at[which, g])

    def o_out(g):
        rows = pl.ds(pl.multiple_of(g * GROUP * n_steps, GROUP * n_steps), GROUP * n_steps)
        return pltpu.make_async_copy(ostage.at[rows], o_ref.at[rows], o_sem.at[g])

    def start_in(g, c):
        cache_in(g, 0).start()
        cache_in(g, 1).start()
        return c

    lax.fori_loop(0, n_groups, start_in, 0)

    ri = lax.broadcasted_iota(jnp.int32, (qrows, rows_kv), 0)
    ci = lax.broadcasted_iota(jnp.int32, (qrows, rows_kv), 1)
    row_kv = ri // (qrows // kv)
    thr[...] = jnp.where(ci % kv == row_kv, ci - kv * (ri % n_steps), 1 << 24)

    def set_pos(b, c):
        for i in range(n_steps):
            cos[pl.ds(b * n_steps + i, 1), :] = jnp.full((1, hd), start_ref[b] + i, jnp.int32).astype(F32)
        return c

    lax.fori_loop(0, n_batch, set_pos, 0)
    trows = 64
    low = lax.broadcasted_iota(jnp.int32, (trows, hd), 1) < hd // 2

    def table(i, c):
        rows = pl.ds(pl.multiple_of(i * trows, trows), trows)
        angle = cos[rows, :] * freq_ref[...]
        s = jnp.sin(angle)
        sin[rows, :] = jnp.where(low, -s, s)
        cos[rows, :] = jnp.cos(angle)
        return c

    lax.fori_loop(0, n_rows // trows, table, 0)

    for j in range(d_model // 128):
        gain[:, j * 128:(j + 1) * 128] = jnp.broadcast_to(norm_ref[j:j + 1, :].astype(F32), (8, 128))

    hid_cp.wait()
    chunk = 16

    def norm_rows(i, c):
        for u in range(4):
            rows = pl.ds(pl.multiple_of(i * 4 * chunk + u * chunk, chunk), chunk)
            x = hid[rows, :].astype(F32)
            inv = lax.rsqrt(jnp.mean(x * x, axis=-1, keepdims=True) + NORM_EPS)
            x = x * inv
            normed[rows, :] = jnp.concatenate([x[:8] * gain[...], x[8:] * gain[...]], axis=0).astype(BF16)
        return c

    lax.fori_loop(0, n_rows // (4 * chunk), norm_rows, 0)

    pi = lax.broadcasted_iota(jnp.int32, (n_rows, n_rows), 0)
    pj = lax.broadcasted_iota(jnp.int32, (n_rows, n_rows), 1)
    perm = jnp.where(pj == (pi % n_steps) * n_batch + pi // n_steps, 1.0, 0.0).astype(BF16)
    for j in range(d_model // 256):
        sl = slice(j * 256, (j + 1) * 256)
        hid[:, sl] = dot(perm, normed[:, sl]).astype(BF16)

    def norm_rope(x, g, rows):
        inv = lax.rsqrt(jnp.mean(x * x, axis=-1, keepdims=True) + NORM_EPS)
        x = x * inv * g
        return (x * cos[rows, :] + pltpu.roll(x, hd // 2, 1) * sin[rows, :]).astype(BF16).astype(F32)

    qg = qg_ref[...].astype(F32)
    kg = kg_ref[...].astype(F32)

    def post(i):
        for r in range(n_rows // 64):
            rows = slice(r * 64, (r + 1) * 64)
            for h in range(2):
                x = raw[i % 2, rows, h * hd:(h + 1) * hd]
                if i < n_q:
                    qs[rows, i * 256 + h * hd:i * 256 + (h + 1) * hd] = norm_rope(x, qg, rows)
                elif i == n_q:
                    ks[rows, h * hd:(h + 1) * hd] = norm_rope(x, kg, rows)
                else:
                    vs[rows, h * hd:(h + 1) * hd] = x.astype(BF16).astype(F32)

    for i in range(n_q + 3):
        if i < n_q + 2:
            w_cps[i].wait()
            w = wq[:, i * 256:(i + 1) * 256] if i < n_q else (wk[...] if i == n_q else wv[...])
            raw[i % 2] = dot(hid[...], w)
        if i > 0:
            post(i - 1)

    scale = hd ** -0.5
    grows = GROUP * n_steps
    lane = lax.broadcasted_iota(jnp.int32, (grows, STATS), 1)
    win_rows = lax.broadcasted_iota(jnp.int32, (32, hd), 0)

    def group_step(g, c):
        cache_in(g, 0).wait()
        cache_in(g, 1).wait()
        rows = pl.ds(pl.multiple_of(g * grows, grows), grows)
        q_slab = qs[rows, :]
        offs = []
        for r in range(GROUP):
            b = g * GROUP + r
            off = kv * (start_ref[b] - blk_start)
            offs.append(off)
            win = pl.multiple_of(jnp.clip((off // 16) * 16, 0, rows_kv - 32), 16)
            for buf, new_ref in ((kbuf, ks), (vbuf, vs)):
                slab = new_ref[rows, :]
                cur = buf[b, pl.ds(win, 32), :].astype(F32)
                for j in range(n_steps):
                    for h in range(kv):
                        new = slab[r * n_steps + j:r * n_steps + j + 1, h * hd:(h + 1) * hd]
                        cur = jnp.where(win_rows == off + kv * j + h - win, new, cur)
                buf[b, pl.ds(win, 32), :] = cur.astype(BF16)
        scores = []
        for r in range(GROUP):
            q = jnp.concatenate([q_slab[r * n_steps:(r + 1) * n_steps, h * hd:(h + 1) * hd] for h in range(heads)], axis=0)
            scores.append(lax.dot_general(q.astype(BF16), kbuf[g * GROUP + r], (((1,), (1,)), ((), ())),
                                          preferred_element_type=F32))
        probs, maxes, sums = [], [], []
        for r in range(GROUP):
            keep = thr[...] <= offs[r] + kv - 1
            s = jnp.where(keep, scores[r] * scale, NEG)
            m = jnp.max(s, axis=-1, keepdims=True)
            p = jnp.where(keep, jnp.exp(s - m), 0.0)
            sums.append(jnp.sum(p, axis=-1, keepdims=True))
            maxes.append(m)
            probs.append(p.astype(BF16))
        outs = [dot(probs[r], vbuf[g * GROUP + r]) for r in range(GROUP)]
        stats = jnp.zeros((grows, STATS), F32)
        for h in range(heads):
            sl = slice(h * n_steps, (h + 1) * n_steps)
            ostage[rows, h * hd:(h + 1) * hd] = jnp.concatenate([o[sl] for o in outs], axis=0)
            stats = jnp.where(lane == h, jnp.concatenate([m[sl] for m in maxes], axis=0), stats)
            stats = jnp.where(lane == heads + h, jnp.concatenate([t[sl] for t in sums], axis=0), stats)
        ostage[rows, heads * hd:] = stats
        cache_out(g, 0).start()
        cache_out(g, 1).start()
        o_out(g).start()
        return c

    lax.fori_loop(0, n_groups, group_step, 0)

    def drain(g, c):
        cache_out(g, 0).wait()
        cache_out(g, 1).wait()
        o_out(g).wait()
        return c

    lax.fori_loop(0, n_groups, drain, 0)


def attention(start_pos, hidden, freq, attn_norm, q_gain, k_gain, w_q, w_k, w_v, k_cache, v_cache):
    n_rows, d_model = hidden.shape
    n_batch, rows_kv, hd = k_cache.shape
    heads = w_q.shape[1] // hd
    n_groups = n_batch // GROUP
    n_steps = n_rows // n_batch
    n_w = w_q.shape[1] // 256 + 2
    width = heads * hd + STATS
    vmem = pl.BlockSpec(memory_space=pltpu.VMEM)
    hbm = pl.BlockSpec(memory_space=pl.ANY)
    return pl.pallas_call(
        attn_kernel,
        out_shape=(jax.ShapeDtypeStruct((n_rows, width), F32),
                   jax.ShapeDtypeStruct(k_cache.shape, BF16), jax.ShapeDtypeStruct(v_cache.shape, BF16)),
        in_specs=[pl.BlockSpec(memory_space=pltpu.SMEM), hbm, vmem, vmem, vmem, vmem, hbm, hbm, hbm, hbm, hbm],
        out_specs=(hbm, hbm, hbm),
        scratch_shapes=[
            pltpu.VMEM((n_rows, d_model), BF16), pltpu.VMEM((n_rows, d_model), BF16),
            pltpu.VMEM(w_q.shape, BF16), pltpu.VMEM(w_k.shape, BF16), pltpu.VMEM(w_v.shape, BF16),
            pltpu.VMEM(k_cache.shape, BF16), pltpu.VMEM(v_cache.shape, BF16),
            pltpu.VMEM((n_rows, hd), F32), pltpu.VMEM((n_rows, hd), F32), pltpu.VMEM((2, n_rows, 256), F32),
            pltpu.VMEM((n_rows, w_q.shape[1]), F32), pltpu.VMEM((n_rows, w_k.shape[1]), F32),
            pltpu.VMEM((n_rows, w_v.shape[1]), F32), pltpu.VMEM((n_rows, width), F32),
            pltpu.VMEM((heads * n_steps, rows_kv), jnp.int32), pltpu.VMEM((8, d_model), F32),
            pltpu.SemaphoreType.DMA, pltpu.SemaphoreType.DMA((n_w,)),
            pltpu.SemaphoreType.DMA((2, n_groups)), pltpu.SemaphoreType.DMA((2, n_groups)),
            pltpu.SemaphoreType.DMA((n_groups,)),
        ],
        compiler_params=pltpu.CompilerParams(vmem_limit_bytes=60_000_000),
        name="attn",
    )(start_pos, hidden, freq, attn_norm, q_gain, k_gain, w_q, w_k, w_v, k_cache, v_cache)


def mlp_kernel(o_ref, hid_ref, norm_ref, wo_ref, wg_ref, wu_ref, wd_ref,
               out_ref,
               x, wo, wg, wu, wd, loc, dbuf, ysend, yrecv, attn, pbuf, in_leaf, in_mid, tbuf, rbuf, mlp_in, act, fbuf, fy, fd,
               x_sem, w_sem, l_sem, d_ssem, d_rsem, y_ssem, y_rsem,
               up_s, up_r, mid_s, mid_r, dn_s, dn_r, fy_s, fy_r, fd_s, fd_r):
    me = lax.axis_index('sp')
    tp = lax.axis_index('tp')
    core = me % 2
    mate = me + 1 - 2 * core
    oth = (me + 2) % 4
    mate_oth = (mate + 2) % 4
    side = tp + 1 - 2 * (tp % 2)
    mid = 3 - tp
    inner = jnp.logical_or(tp == 1, tp == 2)
    leaf = jnp.logical_or(tp == 0, tp == 3)

    n_half, n_rows, d_model = x.shape
    n_pieces = d_model // PIECE
    width = loc.shape[2]
    hd = 128
    heads = (width - STATS) // hd
    n_chunks = dbuf.shape[1]
    crows = dbuf.shape[2]
    n_steps = out_ref.shape[0]
    n_req = n_rows // n_steps
    blk_req = n_req * n_half

    w_cps = [pltpu.make_async_copy(s, d, w_sem.at[i]) for i, (s, d) in
             enumerate(((wo_ref, wo), (wg_ref, wg), (wu_ref, wu), (wd_ref, wd)))]
    l_cps = [pltpu.make_async_copy(o_ref.at[oth], loc.at[0], l_sem.at[0]),
             pltpu.make_async_copy(o_ref.at[me], loc.at[1], l_sem.at[1])]
    x_cps = [pltpu.make_async_copy(
        hid_ref.at[i, pl.ds(pl.multiple_of(me * blk_req + h * n_req, n_req), n_req), :],
        x.at[h, pl.ds(i * n_req, n_req), :], x_sem.at[h, i]) for h in range(n_half) for i in range(n_steps)]
    for cp in l_cps:
        cp.start()
    w_cps[0].start()
    for cp in x_cps:
        cp.start()

    barrier = pltpu.get_barrier_semaphore()
    for dev in ({'sp': mate}, {'sp': oth}, {'tp': side}):
        pl.semaphore_signal(barrier, inc=1, device_id=dev, device_id_type=MESH)

    @pl.when(inner)
    def _():
        pl.semaphore_signal(barrier, inc=1, device_id={'tp': mid}, device_id_type=MESH)
        pl.semaphore_wait(barrier, 4)

    @pl.when(leaf)
    def _():
        pl.semaphore_wait(barrier, 3)

    def remote(src, dst, ssem, rsem, dev):
        return pltpu.make_async_remote_copy(src_ref=src, dst_ref=dst, send_sem=ssem, recv_sem=rsem,
                                            device_id=dev, device_id_type=MESH)

    def d_copy(which, i):
        blk = (mate_oth, mate)[which]
        return remote(o_ref.at[blk, pl.ds(i * crows, crows), :], dbuf.at[which, i], d_ssem.at[which, i], d_rsem.at[which, i],
                      {'sp': mate})

    def y_copy(i):
        return remote(ysend.at[i], yrecv.at[i], y_ssem.at[i], y_rsem.at[i], {'sp': oth})

    for which in range(2):
        for i in range(n_chunks):
            d_copy(which, i).start()

    aw = heads * hd

    def weights(parts):
        m = functools.reduce(jnp.maximum, parts)
        es = [jnp.exp(s - m) for s in parts]
        tot = sum(e * pltpu.roll(s, STATS - heads, 1) for e, s in zip(es, parts))
        return m, es, tot

    stat_lane = lax.broadcasted_iota(jnp.int32, (crows, STATS), 1)
    l_cps[0].wait()
    for i in range(n_chunks):
        d_copy(0, i).wait_recv()
        rs = slice(i * crows, (i + 1) * crows)
        m, (ea, eb), tot = weights((loc[0, rs, aw:], dbuf[0, i, :, aw:]))
        for h in range(heads):
            sl = slice(h * hd, (h + 1) * hd)
            ysend[i, :, sl] = loc[0, rs, sl] * ea[:, h:h + 1] + dbuf[0, i, :, sl] * eb[:, h:h + 1]
        ysend[i, :, aw:] = jnp.where(stat_lane < heads, m, pltpu.roll(tot, heads, 1))
        y_copy(i).start()
    l_cps[1].wait()
    for i in range(n_chunks):
        d_copy(1, i).wait_recv()
    for cp in w_cps[1:]:
        cp.start()

    pi = lax.broadcasted_iota(jnp.int32, (n_rows, n_rows), 0)
    pj = lax.broadcasted_iota(jnp.int32, (n_rows, n_rows), 1)
    perm = jnp.where(pj == (pi % n_req) * n_steps + pi // n_req, 1.0, 0.0).astype(BF16)

    def attn_half(hf):
        per = n_chunks // n_half
        for c in range(per):
            i = hf * per + c
            y_copy(i).wait_recv()
            rs = slice(i * crows, (i + 1) * crows)
            _, es, tot = weights((loc[1, rs, aw:], dbuf[1, i, :, aw:], yrecv[i, :, aw:]))
            inv = 1.0 / tot
            ea, eb, ec = [e * inv for e in es]
            for h in range(heads):
                sl = slice(h * hd, (h + 1) * hd)
                val = (loc[1, rs, sl] * ea[:, h:h + 1] + dbuf[1, i, :, sl] * eb[:, h:h + 1]
                       + yrecv[i, :, sl] * ec[:, h:h + 1])
                attn[hf, c * crows:(c + 1) * crows, sl] = val.astype(BF16)
        attn[hf] = dot(perm, attn[hf]).astype(BF16)

    def up(a, u):
        return remote(pbuf.at[a, u], in_leaf.at[a, u], up_s.at[a, u], up_r.at[a, u], {'tp': side})

    def across(a, u):
        return remote(pbuf.at[a, u], in_mid.at[a, u], mid_s.at[a, u], mid_r.at[a, u], {'tp': mid})

    def down(a, u):
        return remote(tbuf.at[a, u], tbuf.at[a, u], dn_s.at[a, u], dn_r.at[a, u], {'tp': side})

    def cols(k):
        if isinstance(k, int):
            return pl.ds(k * PIECE, PIECE)
        return pl.ds(pl.multiple_of(k * PIECE, PIECE), PIECE)

    def part(a, hf, k):
        left, right = ((attn, wo), (act, wd))[a]
        pbuf[a, hf * n_pieces + k] = dot(left[hf], right[:, cols(k)])

    def stage_a(a, u):
        up(a, u).wait_recv()
        pbuf[a, u] = pbuf[a, u] + in_leaf[a, u]
        across(a, u).start()

    def stage_b(a, u):
        across(a, u).wait_recv()
        tbuf[a, u] = pbuf[a, u] + in_mid[a, u]
        down(a, u).start()
        if a == 1:
            finish_out(u)

    def loop(lo, hi, body):
        def step(k, c):
            body(k)
            return c
        lax.fori_loop(lo, hi, step, 0)

    def norm_half(hf):
        base = hf * n_pieces

        @pl.when(leaf)
        def _():
            loop(0, n_pieces, lambda k: down(0, base + k).wait_recv())
        sq = jnp.zeros((n_rows, 128), F32)
        for k in range(n_pieces):
            r = (x[hf, :, cols(k)].astype(F32) + tbuf[0, base + k]).astype(BF16).astype(F32)
            rbuf[base + k] = r
            for j in range(PIECE // 128):
                piece = r[:, j * 128:(j + 1) * 128]
                sq = sq + piece * piece
        inv = lax.rsqrt(jnp.sum(sq, axis=-1, keepdims=True) * (1.0 / d_model) + NORM_EPS)
        for k in range(n_pieces):
            for j in range(PIECE // 128):
                c0 = k * PIECE + j * 128
                g = norm_ref[c0 // 128:c0 // 128 + 1, :].astype(F32)
                mlp_in[hf, :, c0:c0 + 128] = (rbuf[base + k, :, j * 128:(j + 1) * 128] * inv * g).astype(BF16)

    ffn = wg.shape[1]
    blocks = [(c, min(GU_BLOCK, ffn - c)) for c in range(0, ffn, GU_BLOCK)]
    def gate_up(hf, serve):
        for j, (c0, size) in enumerate(blocks):
            sl = slice(c0, c0 + size)
            gate = dot(mlp_in[hf], wg[:, sl])
            upv = dot(mlp_in[hf], wu[:, sl])
            act[hf, :, sl] = (gate * (1.0 / (1.0 + jnp.exp(-gate))) * upv).astype(BF16)

            late = range(j * LAG // len(blocks), (j + 1) * LAG // len(blocks))
            if len(late):
                @pl.when(inner)
                def _():
                    for i in late:
                        serve(i)

    def put(blk, hf, k, val):
        val = val.astype(BF16)
        for i in range(n_steps):
            out_ref[i, pl.ds(pl.multiple_of(blk * blk_req + hf * n_req, n_req), n_req), cols(k)] = val[i * n_req:(i + 1) * n_req]

    def f_y(u):
        return remote(fbuf.at[u], fy.at[u], fy_s.at[u], fy_r.at[u], {'sp': oth})

    def f_d(which, u):
        src = (fbuf, fy)[which]
        return remote(src.at[u], fd.at[which, u], fd_s.at[which, u], fd_r.at[which, u], {'sp': mate})

    def forward(u):
        f_y(u).wait_recv()
        f_d(1, u).start()
        put(oth, u // n_pieces, u % n_pieces, fy[u])

    def finish_out(u):
        val = (rbuf[u] + tbuf[1, u]).astype(BF16)
        fbuf[u] = val.astype(F32)
        f_y(u).start()
        f_d(0, u).start()
        put(me, u // n_pieces, u % n_pieces, val)
        if isinstance(u, int):
            if u >= FLAG:
                forward(u - FLAG)
        else:
            @pl.when(u >= FLAG)
            def _():
                forward(u - FLAG)

    w_cps[0].wait()
    attn_half(0)

    @pl.when(leaf)
    def _():
        def body(k):
            part(0, 0, k)
            up(0, k).start()
        loop(0, n_pieces, body)

    @pl.when(inner)
    def _():
        def head(k):
            part(0, 0, k)
            stage_a(0, k)
        loop(0, LAG, head)

        def body(k):
            head(k)
            stage_b(0, k - LAG)
        loop(LAG, n_pieces, body)
        if FLUSH:
            loop(n_pieces - LAG, n_pieces, lambda u: stage_b(0, u))

    attn_half(1)

    @pl.when(leaf)
    def _():
        def body(k):
            part(0, 1, k)
            up(0, n_pieces + k).start()
        loop(0, n_pieces, body)

    @pl.when(inner)
    def _():
        def head(k):
            part(0, 1, k)
            stage_a(0, n_pieces + k)

        def body(k):
            head(k)
            stage_b(0, n_pieces - LAG + k)
        loop(0, LAG, head if FLUSH else body)
        loop(LAG, n_pieces, body)

    for cp in x_cps:
        cp.wait()
    norm_half(0)
    w_cps[1].wait()
    w_cps[2].wait()

    gate_up(0, lambda j: stage_b(0, 2 * n_pieces - LAG + j))
    w_cps[3].wait()

    @pl.when(leaf)
    def _():
        def body(k):
            part(1, 0, k)
            up(1, k).start()
        loop(0, n_pieces, body)

    @pl.when(inner)
    def _():
        def head(k):
            part(1, 0, k)
            stage_a(1, k)
        loop(0, LAG, head)

        def body(k):
            head(k)
            stage_b(1, k - LAG)
        loop(LAG, n_pieces, body)

    norm_half(1)

    gate_up(1, lambda j: stage_b(1, n_pieces - LAG + j))

    @pl.when(leaf)
    def _():
        def body(k):
            part(1, 1, k)
            up(1, n_pieces + k).start()
        loop(0, n_pieces, body)

        def tail(u):
            down(1, u).wait_recv()
            finish_out(u)
        loop(0, 2 * n_pieces, tail)

    @pl.when(inner)
    def _():
        def head(k):
            part(1, 1, k)
            stage_a(1, n_pieces + k)
        loop(0, LAG, head)

        def body(k):
            head(k)
            stage_b(1, n_pieces + k - LAG)
        loop(LAG, n_pieces, body)
        loop(2 * n_pieces - LAG, 2 * n_pieces, lambda u: stage_b(1, u))

    loop(2 * n_pieces - FLAG, 2 * n_pieces, forward)

    for hf in range(n_half):
        def last(k, hf=hf):
            u = hf * n_pieces + k
            f_d(0, u).wait_recv()
            put(mate, hf, k, fd[0, u])
            f_d(1, u).wait_recv()
            put(mate_oth, hf, k, fd[1, u])
        loop(0, n_pieces, last)

    for which in range(2):
        for i in range(n_chunks):
            d_copy(which, i).wait_send()
    for i in range(n_chunks):
        y_copy(i).wait_send()

    def sends(u):
        f_y(u).wait_send()
        f_d(0, u).wait_send()
        f_d(1, u).wait_send()
        for a in range(2):
            @pl.when(leaf)
            def _():
                up(a, u).wait_send()

            @pl.when(inner)
            def _():
                across(a, u).wait_send()
                down(a, u).wait_send()
    loop(0, n_half * n_pieces, sends)


def mlp(o_part, hidden, mlp_norm, w_o, w_gate, w_up, w_down):
    n_blk, blk_rows, width = o_part.shape
    n_steps, n_batch, d_model = hidden.shape
    n_half = 2
    n_rows = blk_rows // n_half
    n_pieces = d_model // PIECE
    n_chunks = 4
    crows = blk_rows // n_chunks
    ffn = w_gate.shape[1]
    vmem = pl.BlockSpec(memory_space=pltpu.VMEM)
    hbm = pl.BlockSpec(memory_space=pl.ANY)
    dma = pltpu.SemaphoreType.DMA
    n_u = n_half * n_pieces
    piece = (n_u, n_rows, PIECE)
    return pl.pallas_call(
        mlp_kernel,
        out_shape=jax.ShapeDtypeStruct(hidden.shape, BF16),
        in_specs=[hbm, hbm, vmem, hbm, hbm, hbm, hbm],
        out_specs=vmem,
        scratch_shapes=[
            pltpu.VMEM((n_half, n_rows, d_model), BF16),
            pltpu.VMEM(w_o.shape, BF16), pltpu.VMEM(w_gate.shape, BF16),
            pltpu.VMEM(w_up.shape, BF16), pltpu.VMEM(w_down.shape, BF16),
            pltpu.VMEM((2, blk_rows, width), F32), pltpu.VMEM((2, n_chunks, crows, width), F32),
            pltpu.VMEM((n_chunks, crows, width), F32), pltpu.VMEM((n_chunks, crows, width), F32),
            pltpu.VMEM((n_half, n_rows, w_o.shape[0]), BF16),
            pltpu.VMEM((2,) + piece, F32), pltpu.VMEM((2,) + piece, F32),
            pltpu.VMEM((2,) + piece, F32), pltpu.VMEM((2,) + piece, F32),
            pltpu.VMEM(piece, F32), pltpu.VMEM((n_half, n_rows, d_model), BF16), pltpu.VMEM((n_half, n_rows, ffn), BF16),
            pltpu.VMEM(piece, F32), pltpu.VMEM(piece, F32), pltpu.VMEM((2,) + piece, F32),
            dma((n_half, n_steps)), dma((4,)), dma((2,)),
            dma((2, n_chunks)), dma((2, n_chunks)), dma((n_chunks,)), dma((n_chunks,)),
            dma((2, n_u)), dma((2, n_u)), dma((2, n_u)), dma((2, n_u)), dma((2, n_u)), dma((2, n_u)),
            dma((n_u,)), dma((n_u,)), dma((2, n_u)), dma((2, n_u)),
        ],
        compiler_params=pltpu.CompilerParams(vmem_limit_bytes=VMEM_LIMIT, collective_id=0, has_side_effects=True),
        name="combine_mlp",
    )(o_part, hidden, mlp_norm, w_o, w_gate, w_up, w_down)


def solution(mesh):
    cache_spec = P('dp', 'sp', 'tp', None)
    col_spec = P(None, 'tp')
    row_spec = P('tp', None)
    in_specs = (P(None, 'dp', None), P('dp'), cache_spec, cache_spec, col_spec, col_spec, col_spec, row_spec,
                col_spec, col_spec, row_spec, P(), P(), P(), P())
    out_specs = (P(None, 'dp', None), cache_spec, cache_spec)

    def shard_body(hidden, start_pos, k_cache, v_cache, w_q, w_k, w_v, w_o, w_gate, w_up, w_down, attn_norm, mlp_norm, q_gain, k_gain):
        n_steps, n_batch, d_model = hidden.shape
        _, seq, kv, hd = k_cache.shape
        half = np.arange(hd // 2)
        freq = ROPE_BASE ** (-half * (2.0 / hd))
        freq = jnp.asarray(np.concatenate([freq, freq])[None], F32)
        o_part, k_out, v_out = attention(
            start_pos, hidden.reshape(-1, d_model), freq, attn_norm.reshape(-1, 128), q_gain[None], k_gain[None],
            w_q, w_k, w_v, k_cache.reshape(n_batch, seq * kv, hd), v_cache.reshape(n_batch, seq * kv, hd))
        n_sp = 4
        out = mlp(o_part.reshape(n_sp, -1, o_part.shape[1]), hidden, mlp_norm.reshape(-1, 128), w_o, w_gate, w_up, w_down)
        return out, k_out.reshape(k_cache.shape), v_out.reshape(v_cache.shape)

    return jax.shard_map(shard_body, mesh=mesh, in_specs=in_specs, out_specs=out_specs, check_vma=False)
```

```python
import functools
import jax
import jax.numpy as jnp
import numpy as np
from jax import lax
from jax.experimental import pallas as pl
from jax.experimental.pallas import tpu as pltpu
from jax.sharding import PartitionSpec as P

ROPE_BASE = 1000000.0
NORM_EPS = 1e-06
LOWEST = float(np.finfo(np.float32).min)
LOG2E = 1.4426950408889634
F32 = jnp.float32
BF16 = jnp.bfloat16
MESH = pl.DeviceIdType.MESH
STATS = 128
GROUP = 8
PIECE = 256
LAG = 4
FLAG = 4
GU_BLOCK = 384
PAIR = 2
VMEM_LIMIT = 66_900_000


def dot(a, b):
    return jnp.dot(a, b, preferred_element_type=F32)


def attn_kernel(start_ref, hid_ref, freq_ref, norm_ref, qg_ref, kg_ref, wq_ref, wk_ref, wv_ref, kc_ref, vc_ref,
                o_ref, ko_ref, vo_ref,
                hid, normed, wq, wk, wv, kbuf, vbuf, cos, sin, raw, qs, ks, vs, ostage, thr, gain,
                hid_sem, w_sem, in_sem, out_sem, o_sem):
    n_rows, d_model = hid.shape
    n_batch, rows_kv, hd = kbuf.shape
    n_steps = n_rows // n_batch
    heads = wq.shape[1] // hd
    kv = wk.shape[1] // hd
    seq = rows_kv // kv
    n_groups = n_batch // GROUP
    qrows = heads * n_steps
    blk_start = lax.axis_index('sp') * seq

    hid_cp = pltpu.make_async_copy(hid_ref, hid, hid_sem)
    hid_cp.start()
    n_q = wq.shape[1] // 256
    w_cps = []
    for i in range(n_q):
        w_cps.append(pltpu.make_async_copy(wq_ref.at[:, pl.ds(i * 256, 256)], wq.at[:, pl.ds(i * 256, 256)], w_sem.at[i]))
    w_cps.append(pltpu.make_async_copy(wk_ref, wk, w_sem.at[n_q]))
    w_cps.append(pltpu.make_async_copy(wv_ref, wv, w_sem.at[n_q + 1]))
    w_cps[0].start()

    def cache_in(g, which):
        src, dst = ((kc_ref, kbuf), (vc_ref, vbuf))[which]
        rows = pl.ds(g * GROUP, GROUP)
        return pltpu.make_async_copy(src.at[rows], dst.at[rows], in_sem.at[which, g])

    def cache_out(g, which):
        src, dst = ((kbuf, ko_ref), (vbuf, vo_ref))[which]
        rows = pl.ds(g * GROUP, GROUP)
        return pltpu.make_async_copy(src.at[rows], dst.at[rows], out_sem.at[which, g])

    def o_out(g):
        rows = pl.ds(pl.multiple_of(g * GROUP * n_steps, GROUP * n_steps), GROUP * n_steps)
        return pltpu.make_async_copy(ostage.at[rows], o_ref.at[rows], o_sem.at[g])

    def start_in(g, c):
        cache_in(g, 0).start()
        cache_in(g, 1).start()
        return c

    ri = lax.broadcasted_iota(jnp.int32, (qrows, rows_kv), 0)
    ci = lax.broadcasted_iota(jnp.int32, (qrows, rows_kv), 1)
    row_kv = ri // (qrows // kv)
    thr[...] = jnp.where(ci % kv == row_kv, ci - kv * (ri % n_steps), 1 << 24)

    def set_pos(b, c):
        for i in range(n_steps):
            cos[pl.ds(b * n_steps + i, 1), :] = jnp.full((1, hd), start_ref[b] + i, jnp.int32).astype(F32)
        return c

    lax.fori_loop(0, n_batch, set_pos, 0)
    trows = 64
    low = lax.broadcasted_iota(jnp.int32, (trows, hd), 1) < hd // 2

    def table(i, c):
        rows = pl.ds(pl.multiple_of(i * trows, trows), trows)
        angle = cos[rows, :] * freq_ref[...]
        s = jnp.sin(angle)
        sin[rows, :] = jnp.where(low, -s, s)
        cos[rows, :] = jnp.cos(angle)
        return c

    lax.fori_loop(0, n_rows // trows, table, 0)

    for j in range(d_model // 128):
        gain[:, j * 128:(j + 1) * 128] = jnp.broadcast_to(norm_ref[j:j + 1, :].astype(F32), (8, 128))

    hid_cp.wait()
    for cp in w_cps[1:]:
        cp.start()
    chunk = 16

    def norm_rows(i, c):
        for u in range(4):
            rows = pl.ds(pl.multiple_of(i * 4 * chunk + u * chunk, chunk), chunk)
            sq = jnp.zeros((chunk, 128), F32)
            for j in range(d_model // 128):
                x = hid[rows, j * 128:(j + 1) * 128].astype(F32)
                sq = sq + x * x
            inv = lax.rsqrt(jnp.sum(sq, axis=-1, keepdims=True) * (1.0 / d_model) + NORM_EPS)
            for j in range(d_model // 128):
                sl = slice(j * 128, (j + 1) * 128)
                x = hid[rows, sl].astype(F32) * inv
                normed[rows, sl] = jnp.concatenate([x[:8] * gain[:, sl], x[8:] * gain[:, sl]], axis=0).astype(BF16)
        return c

    lax.fori_loop(0, n_rows // (4 * chunk), norm_rows, 0)

    pi = lax.broadcasted_iota(jnp.int32, (n_rows, n_rows), 0)
    pj = lax.broadcasted_iota(jnp.int32, (n_rows, n_rows), 1)
    perm = jnp.where(pj == (pi % n_steps) * n_batch + pi // n_steps, 1.0, 0.0).astype(BF16)
    for j in range(d_model // 256):
        sl = slice(j * 256, (j + 1) * 256)
        hid[:, sl] = dot(perm, normed[:, sl]).astype(BF16)

    def norm_rope(x, g, rows):
        inv = lax.rsqrt(jnp.mean(x * x, axis=-1, keepdims=True) + NORM_EPS)
        x = x * inv * g
        return (x * cos[rows, :] + pltpu.roll(x, hd // 2, 1) * sin[rows, :]).astype(BF16).astype(F32)

    qg = qg_ref[...].astype(F32)
    kg = kg_ref[...].astype(F32)

    def post(i):
        for r in range(n_rows // 64):
            rows = slice(r * 64, (r + 1) * 64)
            for h in range(2):
                x = raw[i % 2, rows, h * hd:(h + 1) * hd]
                if i < n_q:
                    qs[rows, i * 256 + h * hd:i * 256 + (h + 1) * hd] = norm_rope(x, qg, rows)
                elif i == n_q:
                    ks[pl.ds(r * 64 * kv + h, 64, stride=kv), :] = norm_rope(x, kg, rows)
                else:
                    vs[pl.ds(r * 64 * kv + h, 64, stride=kv), :] = x.astype(BF16).astype(F32)

    for i in range(n_q + 3):
        if i < n_q + 2:
            w_cps[i].wait()
            for g in range(n_groups * i // (n_q + 2), n_groups * (i + 1) // (n_q + 2)):
                start_in(g, 0)
            w = wq[:, i * 256:(i + 1) * 256] if i < n_q else (wk[...] if i == n_q else wv[...])
            for r in range(2):
                rr = slice(r * n_rows // 2, (r + 1) * n_rows // 2)
                raw[i % 2, rr] = dot(hid[rr], w)
        if i > 0:
            post(i - 1)

    scale = hd ** -0.5
    grows = GROUP * n_steps
    lane = lax.broadcasted_iota(jnp.int32, (grows, STATS), 1)
    win_rows = lax.broadcasted_iota(jnp.int32, (32, hd), 0)

    def group_step(g, c):
        cache_in(g, 0).wait()
        cache_in(g, 1).wait()
        rows = pl.ds(pl.multiple_of(g * grows, grows), grows)
        q_slab = qs[rows, :]
        offs = []
        for r in range(GROUP):
            b = g * GROUP + r
            off = kv * (start_ref[b] - blk_start)
            offs.append(off)
            win = pl.multiple_of(jnp.clip((off // 16) * 16, 0, rows_kv - 32), 16)
            n_new = n_steps * kv
            at = win_rows + (win - off)
            hit = jnp.logical_and(at >= 0, at < n_new)
            for buf, new_ref in ((kbuf, ks), (vbuf, vs)):
                new = pltpu.roll(new_ref[pl.ds(pl.multiple_of(b * n_new, n_new), n_new), :], off % n_new, 0)
                cur = buf[b, pl.ds(win, 32), :].astype(F32)
                cur = jnp.where(hit, jnp.concatenate([new] * (32 // n_new), axis=0), cur)
                buf[b, pl.ds(win, 32), :] = cur.astype(BF16)
        scores = []
        for r in range(GROUP):
            q = jnp.concatenate([q_slab[r * n_steps:(r + 1) * n_steps, h * hd:(h + 1) * hd] for h in range(heads)], axis=0)
            scores.append(lax.dot_general(q.astype(BF16), kbuf[g * GROUP + r], (((1,), (1,)), ((), ())),
                                          preferred_element_type=F32))
        probs, maxes, sums = [], [], []
        for r in range(GROUP):
            s = jnp.where(thr[...] <= offs[r] + kv - 1, scores[r], -jnp.inf)
            m = jnp.maximum(jnp.max(s, axis=-1, keepdims=True), LOWEST)
            p = jnp.exp2((s - m) * (scale * LOG2E))
            sums.append(jnp.sum(p, axis=-1, keepdims=True))
            maxes.append(m * scale)
            probs.append(p.astype(BF16))
        outs = [dot(probs[r], vbuf[g * GROUP + r]) for r in range(GROUP)]
        stats = jnp.zeros((grows, STATS), F32)
        for h in range(heads):
            sl = slice(h * n_steps, (h + 1) * n_steps)
            ostage[rows, h * hd:(h + 1) * hd] = jnp.concatenate([o[sl] for o in outs], axis=0)
            stats = jnp.where(lane == h, jnp.concatenate([m[sl] for m in maxes], axis=0), stats)
            stats = jnp.where(lane == heads + h, jnp.concatenate([t[sl] for t in sums], axis=0), stats)
        ostage[rows, heads * hd:] = stats
        cache_out(g, 0).start()
        cache_out(g, 1).start()
        o_out(g).start()
        return c

    lax.fori_loop(0, n_groups, group_step, 0)

    def drain(g, c):
        cache_out(g, 0).wait()
        cache_out(g, 1).wait()
        o_out(g).wait()
        return c

    lax.fori_loop(0, n_groups, drain, 0)


def attention(start_pos, hidden, freq, attn_norm, q_gain, k_gain, w_q, w_k, w_v, k_cache, v_cache):
    n_rows, d_model = hidden.shape
    n_batch, rows_kv, hd = k_cache.shape
    heads = w_q.shape[1] // hd
    n_groups = n_batch // GROUP
    n_steps = n_rows // n_batch
    n_w = w_q.shape[1] // 256 + 2
    width = heads * hd + STATS
    vmem = pl.BlockSpec(memory_space=pltpu.VMEM)
    hbm = pl.BlockSpec(memory_space=pl.ANY)
    return pl.pallas_call(
        attn_kernel,
        out_shape=(jax.ShapeDtypeStruct((n_rows, width), F32),
                   jax.ShapeDtypeStruct(k_cache.shape, BF16), jax.ShapeDtypeStruct(v_cache.shape, BF16)),
        in_specs=[pl.BlockSpec(memory_space=pltpu.SMEM), hbm, vmem, vmem, vmem, vmem, hbm, hbm, hbm, hbm, hbm],
        out_specs=(hbm, hbm, hbm),
        scratch_shapes=[
            pltpu.VMEM((n_rows, d_model), BF16), pltpu.VMEM((n_rows, d_model), BF16),
            pltpu.VMEM(w_q.shape, BF16), pltpu.VMEM(w_k.shape, BF16), pltpu.VMEM(w_v.shape, BF16),
            pltpu.VMEM(k_cache.shape, BF16), pltpu.VMEM(v_cache.shape, BF16),
            pltpu.VMEM((n_rows, hd), F32), pltpu.VMEM((n_rows, hd), F32), pltpu.VMEM((2, n_rows, 256), F32),
            pltpu.VMEM((n_rows, w_q.shape[1]), F32), pltpu.VMEM((n_rows * w_k.shape[1] // hd, hd), F32),
            pltpu.VMEM((n_rows * w_v.shape[1] // hd, hd), F32), pltpu.VMEM((n_rows, width), F32),
            pltpu.VMEM((heads * n_steps, rows_kv), jnp.int32), pltpu.VMEM((8, d_model), F32),
            pltpu.SemaphoreType.DMA, pltpu.SemaphoreType.DMA((n_w,)),
            pltpu.SemaphoreType.DMA((2, n_groups)), pltpu.SemaphoreType.DMA((2, n_groups)),
            pltpu.SemaphoreType.DMA((n_groups,)),
        ],
        compiler_params=pltpu.CompilerParams(vmem_limit_bytes=60_000_000),
        name="attn",
    )(start_pos, hidden, freq, attn_norm, q_gain, k_gain, w_q, w_k, w_v, k_cache, v_cache)


def mlp_kernel(o_ref, hid_ref, norm_ref, wo_ref, wg_ref, wu_ref, wd_ref,
               out_ref,
               x, wo, wg, wu, wd, loc, dbuf, ysend, yrecv, attn, pbuf, in_leaf, in_mid, tbuf, rbuf, mlp_in, act, fbuf, fy, fd,
               x_sem, w_sem, l_sem, d_ssem, d_rsem, y_ssem, y_rsem,
               up_s, up_r, mid_s, mid_r, dn_s, dn_r, fy_s, fy_r, fd_s, fd_r):
    me = lax.axis_index('sp')
    tp = lax.axis_index('tp')
    core = me % 2
    mate = me + 1 - 2 * core
    oth = (me + 2) % 4
    mate_oth = (mate + 2) % 4
    side = tp + 1 - 2 * (tp % 2)
    mid = 3 - tp
    inner = jnp.logical_or(tp == 1, tp == 2)
    leaf = jnp.logical_or(tp == 0, tp == 3)

    n_half, n_rows, d_model = x.shape
    n_pieces = d_model // PIECE
    width = loc.shape[2]
    hd = 128
    heads = (width - STATS) // hd
    n_chunks = dbuf.shape[1]
    crows = dbuf.shape[2]
    n_steps = out_ref.shape[0]
    n_req = n_rows // n_steps
    blk_req = n_req * n_half

    w_cps = [pltpu.make_async_copy(s, d, w_sem.at[i]) for i, (s, d) in
             enumerate(((wo_ref, wo), (wg_ref, wg), (wu_ref, wu), (wd_ref, wd)))]
    l_cps = [pltpu.make_async_copy(o_ref.at[oth], loc.at[0], l_sem.at[0]),
             pltpu.make_async_copy(o_ref.at[me], loc.at[1], l_sem.at[1])]
    x_cps = [pltpu.make_async_copy(
        hid_ref.at[i, pl.ds(pl.multiple_of(me * blk_req + h * n_req, n_req), n_req), :],
        x.at[h, pl.ds(i * n_req, n_req), :], x_sem.at[h, i]) for h in range(n_half) for i in range(n_steps)]
    for cp in l_cps:
        cp.start()

    barrier = pltpu.get_barrier_semaphore()
    for dev in ({'sp': mate}, {'sp': oth}, {'tp': side}):
        pl.semaphore_signal(barrier, inc=1, device_id=dev, device_id_type=MESH)

    @pl.when(inner)
    def _():
        pl.semaphore_signal(barrier, inc=1, device_id={'tp': mid}, device_id_type=MESH)
        pl.semaphore_wait(barrier, 4)

    @pl.when(leaf)
    def _():
        pl.semaphore_wait(barrier, 3)

    def remote(src, dst, ssem, rsem, dev):
        return pltpu.make_async_remote_copy(src_ref=src, dst_ref=dst, send_sem=ssem, recv_sem=rsem,
                                            device_id=dev, device_id_type=MESH)

    def d_copy(which, i):
        blk = (mate_oth, mate)[which]
        return remote(o_ref.at[blk, pl.ds(i * crows, crows), :], dbuf.at[which, i], d_ssem.at[which, i], d_rsem.at[which, i],
                      {'sp': mate})

    def y_copy(i):
        return remote(ysend.at[i], yrecv.at[i], y_ssem.at[i], y_rsem.at[i], {'sp': oth})

    for which in range(2):
        for i in range(n_chunks):
            d_copy(which, i).start()

    aw = heads * hd

    def weights(parts):
        m = functools.reduce(jnp.maximum, parts)
        es = [jnp.exp(s - m) for s in parts]
        tot = sum(e * pltpu.roll(s, STATS - heads, 1) for e, s in zip(es, parts))
        return m, es, tot

    stat_lane = lax.broadcasted_iota(jnp.int32, (crows, STATS), 1)
    l_cps[0].wait()
    for i in range(n_chunks):
        d_copy(0, i).wait_recv()
        rs = slice(i * crows, (i + 1) * crows)
        m, (ea, eb), tot = weights((loc[0, rs, aw:], dbuf[0, i, :, aw:]))
        for h in range(heads):
            sl = slice(h * hd, (h + 1) * hd)
            ysend[i, :, sl] = loc[0, rs, sl] * ea[:, h:h + 1] + dbuf[0, i, :, sl] * eb[:, h:h + 1]
        ysend[i, :, aw:] = jnp.where(stat_lane < heads, m, pltpu.roll(tot, heads, 1))
        y_copy(i).start()
        if i == 0:
            w_cps[0].start()
            for cp in x_cps:
                cp.start()
    l_cps[1].wait()
    for i in range(n_chunks):
        d_copy(1, i).wait_recv()
    for cp in w_cps[1:]:
        cp.start()

    pi = lax.broadcasted_iota(jnp.int32, (n_rows, n_rows), 0)
    pj = lax.broadcasted_iota(jnp.int32, (n_rows, n_rows), 1)
    perm = jnp.where(pj == (pi % n_req) * n_steps + pi // n_req, 1.0, 0.0).astype(BF16)

    def attn_half(hf):
        per = n_chunks // n_half
        for c in range(per):
            i = hf * per + c
            y_copy(i).wait_recv()
            rs = slice(i * crows, (i + 1) * crows)
            _, es, tot = weights((loc[1, rs, aw:], dbuf[1, i, :, aw:], yrecv[i, :, aw:]))
            inv = 1.0 / tot
            ea, eb, ec = [e * inv for e in es]
            for h in range(heads):
                sl = slice(h * hd, (h + 1) * hd)
                val = (loc[1, rs, sl] * ea[:, h:h + 1] + dbuf[1, i, :, sl] * eb[:, h:h + 1]
                       + yrecv[i, :, sl] * ec[:, h:h + 1])
                attn[hf, c * crows:(c + 1) * crows, sl] = val.astype(BF16)
        attn[hf] = dot(perm, attn[hf]).astype(BF16)

    def up(a, u):
        return remote(pbuf.at[a, u], in_leaf.at[a, u], up_s.at[a, u], up_r.at[a, u], {'tp': side})

    def across(a, u):
        return remote(pbuf.at[a, u], in_mid.at[a, u], mid_s.at[a, u], mid_r.at[a, u], {'tp': mid})

    def down(a, u):
        return remote(tbuf.at[a, u], tbuf.at[a, u], dn_s.at[a, u], dn_r.at[a, u], {'tp': side})

    def cols(k):
        if isinstance(k, int):
            return pl.ds(k * PIECE, PIECE)
        return pl.ds(pl.multiple_of(k * PIECE, PIECE), PIECE)

    def part(a, hf, k):
        left, right = ((attn, wo), (act, wd))[a]
        pbuf[a, hf * n_pieces + k] = dot(left[hf], right[:, cols(k)])

    def stage_a(a, u):
        up(a, u).wait_recv()
        pbuf[a, u] = pbuf[a, u] + in_leaf[a, u]
        across(a, u).start()

    def stage_b(a, u):
        across(a, u).wait_recv()
        tbuf[a, u] = pbuf[a, u] + in_mid[a, u]
        down(a, u).start()
        if a == 1:
            finish_out(u)

    def loop(lo, hi, body):
        def step(k, c):
            body(k)
            return c
        lax.fori_loop(lo, hi, step, 0)

    def parts(a, hf):
        def body(i):
            for k in range(PAIR):
                part(a, hf, i * PAIR + k)

            @pl.when(leaf)
            def _():
                for k in range(PAIR):
                    up(a, hf * n_pieces + i * PAIR + k).start()
        loop(0, n_pieces // PAIR, body)

    def norm_half(hf):
        base = hf * n_pieces

        @pl.when(leaf)
        def _():
            loop(0, n_pieces, lambda k: down(0, base + k).wait_recv())
        sq = jnp.zeros((n_rows, 128), F32)
        for k in range(n_pieces):
            r = (x[hf, :, cols(k)].astype(F32) + tbuf[0, base + k]).astype(BF16).astype(F32)
            rbuf[base + k] = r
            for j in range(PIECE // 128):
                piece = r[:, j * 128:(j + 1) * 128]
                sq = sq + piece * piece
        inv = lax.rsqrt(jnp.sum(sq, axis=-1, keepdims=True) * (1.0 / d_model) + NORM_EPS)
        for k in range(n_pieces):
            for j in range(PIECE // 128):
                c0 = k * PIECE + j * 128
                g = norm_ref[c0 // 128:c0 // 128 + 1, :].astype(F32)
                mlp_in[hf, :, c0:c0 + 128] = (rbuf[base + k, :, j * 128:(j + 1) * 128] * inv * g).astype(BF16)

    ffn = wg.shape[1]
    blocks = [(c, min(GU_BLOCK, ffn - c)) for c in range(0, ffn, GU_BLOCK)]
    def gate_up(hf, serve):
        for j, (c0, size) in enumerate(blocks):
            sl = slice(c0, c0 + size)
            gate = dot(mlp_in[hf], wg[:, sl])
            upv = dot(mlp_in[hf], wu[:, sl])
            act[hf, :, sl] = (gate * (1.0 / (1.0 + jnp.exp(-gate))) * upv).astype(BF16)

            @pl.when(inner)
            def _():
                serve(j)

    def put(blk, hf, k, val):
        val = val.astype(BF16)
        for i in range(n_steps):
            out_ref[i, pl.ds(pl.multiple_of(blk * blk_req + hf * n_req, n_req), n_req), cols(k)] = val[i * n_req:(i + 1) * n_req]

    def f_y(u):
        return remote(fbuf.at[u], fy.at[u], fy_s.at[u], fy_r.at[u], {'sp': oth})

    def f_d(which, u):
        src = (fbuf, fy)[which]
        return remote(src.at[u], fd.at[which, u], fd_s.at[which, u], fd_r.at[which, u], {'sp': mate})

    def forward(u):
        f_y(u).wait_recv()
        f_d(1, u).start()
        put(oth, u // n_pieces, u % n_pieces, fy[u])

    def finish_out(u):
        val = (rbuf[u] + tbuf[1, u]).astype(BF16)
        fbuf[u] = val.astype(F32)
        f_y(u).start()
        f_d(0, u).start()
        put(me, u // n_pieces, u % n_pieces, val)
        if isinstance(u, int):
            if u >= FLAG:
                forward(u - FLAG)
        else:
            @pl.when(u >= FLAG)
            def _():
                forward(u - FLAG)

    w_cps[0].wait()
    attn_half(0)
    parts(0, 0)
    attn_half(1)
    n_u = n_half * n_pieces

    @pl.when(leaf)
    def _():
        parts(0, 1)

    @pl.when(inner)
    def _():
        def head(u):
            part(0, 1, u)
            stage_a(0, u)
        loop(0, LAG, head)

        def body(u):
            head(u)
            stage_b(0, u - LAG)
        loop(LAG, n_pieces, body)

        def rest(u):
            stage_a(0, u)
            stage_b(0, u - LAG)
        loop(n_pieces, n_u, rest)

    for cp in x_cps:
        cp.wait()
    norm_half(0)
    w_cps[1].wait()
    w_cps[2].wait()

    def serve0(j):
        if j < LAG:
            stage_b(0, n_u - LAG + j)
    gate_up(0, serve0)
    w_cps[3].wait()

    parts(1, 0)
    norm_half(1)
    shares = [[int(u) for u in s] for s in np.array_split(np.arange(n_pieces), len(blocks))]

    def serve1(j):
        for u in shares[j]:
            stage_a(1, u)
            if u >= LAG:
                stage_b(1, u - LAG)
    gate_up(1, serve1)
    parts(1, 1)

    @pl.when(leaf)
    def _():
        def take(u):
            down(1, u).wait_recv()
            finish_out(u)
        loop(0, n_u, take)

    @pl.when(inner)
    def _():
        loop(n_pieces - LAG, n_pieces, lambda u: stage_b(1, u))
        loop(n_pieces, n_pieces + LAG, lambda u: stage_a(1, u))

        def body(u):
            stage_a(1, u)
            stage_b(1, u - LAG)
        loop(n_pieces + LAG, n_u, body)
        loop(n_u - LAG, n_u, lambda u: stage_b(1, u))

    loop(2 * n_pieces - FLAG, 2 * n_pieces, forward)

    for hf in range(n_half):
        def last(k, hf=hf):
            u = hf * n_pieces + k
            f_d(0, u).wait_recv()
            put(mate, hf, k, fd[0, u])
            f_d(1, u).wait_recv()
            put(mate_oth, hf, k, fd[1, u])
        loop(0, n_pieces, last)

    for which in range(2):
        for i in range(n_chunks):
            d_copy(which, i).wait_send()
    for i in range(n_chunks):
        y_copy(i).wait_send()

    def sends(u):
        f_y(u).wait_send()
        f_d(0, u).wait_send()
        f_d(1, u).wait_send()
        for a in range(2):
            @pl.when(leaf)
            def _():
                up(a, u).wait_send()

            @pl.when(inner)
            def _():
                across(a, u).wait_send()
                down(a, u).wait_send()
    loop(0, n_half * n_pieces, sends)


def mlp(o_part, hidden, mlp_norm, w_o, w_gate, w_up, w_down):
    n_blk, blk_rows, width = o_part.shape
    n_steps, n_batch, d_model = hidden.shape
    n_half = 2
    n_rows = blk_rows // n_half
    n_pieces = d_model // PIECE
    n_chunks = 4
    crows = blk_rows // n_chunks
    ffn = w_gate.shape[1]
    vmem = pl.BlockSpec(memory_space=pltpu.VMEM)
    hbm = pl.BlockSpec(memory_space=pl.ANY)
    dma = pltpu.SemaphoreType.DMA
    n_u = n_half * n_pieces
    piece = (n_u, n_rows, PIECE)
    return pl.pallas_call(
        mlp_kernel,
        out_shape=jax.ShapeDtypeStruct(hidden.shape, BF16),
        in_specs=[hbm, hbm, vmem, hbm, hbm, hbm, hbm],
        out_specs=vmem,
        scratch_shapes=[
            pltpu.VMEM((n_half, n_rows, d_model), BF16),
            pltpu.VMEM(w_o.shape, BF16), pltpu.VMEM(w_gate.shape, BF16),
            pltpu.VMEM(w_up.shape, BF16), pltpu.VMEM(w_down.shape, BF16),
            pltpu.VMEM((2, blk_rows, width), F32), pltpu.VMEM((2, n_chunks, crows, width), F32),
            pltpu.VMEM((n_chunks, crows, width), F32), pltpu.VMEM((n_chunks, crows, width), F32),
            pltpu.VMEM((n_half, n_rows, w_o.shape[0]), BF16),
            pltpu.VMEM((2,) + piece, F32), pltpu.VMEM((2,) + piece, F32),
            pltpu.VMEM((2,) + piece, F32), pltpu.VMEM((2,) + piece, F32),
            pltpu.VMEM(piece, F32), pltpu.VMEM((n_half, n_rows, d_model), BF16), pltpu.VMEM((n_half, n_rows, ffn), BF16),
            pltpu.VMEM(piece, F32), pltpu.VMEM(piece, F32), pltpu.VMEM((2,) + piece, F32),
            dma((n_half, n_steps)), dma((4,)), dma((2,)),
            dma((2, n_chunks)), dma((2, n_chunks)), dma((n_chunks,)), dma((n_chunks,)),
            dma((2, n_u)), dma((2, n_u)), dma((2, n_u)), dma((2, n_u)), dma((2, n_u)), dma((2, n_u)),
            dma((n_u,)), dma((n_u,)), dma((2, n_u)), dma((2, n_u)),
        ],
        compiler_params=pltpu.CompilerParams(vmem_limit_bytes=VMEM_LIMIT, collective_id=0, has_side_effects=True),
        name="combine_mlp",
    )(o_part, hidden, mlp_norm, w_o, w_gate, w_up, w_down)


def solution(mesh):
    cache_spec = P('dp', 'sp', 'tp', None)
    col_spec = P(None, 'tp')
    row_spec = P('tp', None)
    in_specs = (P(None, 'dp', None), P('dp'), cache_spec, cache_spec, col_spec, col_spec, col_spec, row_spec,
                col_spec, col_spec, row_spec, P(), P(), P(), P())
    out_specs = (P(None, 'dp', None), cache_spec, cache_spec)

    def shard_body(hidden, start_pos, k_cache, v_cache, w_q, w_k, w_v, w_o, w_gate, w_up, w_down, attn_norm, mlp_norm, q_gain, k_gain):
        n_steps, n_batch, d_model = hidden.shape
        _, seq, kv, hd = k_cache.shape
        half = np.arange(hd // 2)
        freq = ROPE_BASE ** (-half * (2.0 / hd))
        freq = jnp.asarray(np.concatenate([freq, freq])[None], F32)
        o_part, k_out, v_out = attention(
            start_pos, hidden.reshape(-1, d_model), freq, attn_norm.reshape(-1, 128), q_gain[None], k_gain[None],
            w_q, w_k, w_v, k_cache.reshape(n_batch, seq * kv, hd), v_cache.reshape(n_batch, seq * kv, hd))
        n_sp = 4
        out = mlp(o_part.reshape(n_sp, -1, o_part.shape[1]), hidden, mlp_norm.reshape(-1, 128), w_o, w_gate, w_up, w_down)
        return out, k_out.reshape(k_cache.shape), v_out.reshape(v_cache.shape)

    return jax.shard_map(shard_body, mesh=mesh, in_specs=in_specs, out_specs=out_specs, check_vma=False)
```

```python
import functools
import jax
import jax.numpy as jnp
import numpy as np
from jax import lax
from jax.experimental import pallas as pl
from jax.experimental.pallas import tpu as pltpu
from jax.sharding import PartitionSpec as P

ROPE_BASE = 1000000.0
NORM_EPS = 1e-06
LOWEST = float(np.finfo(np.float32).min)
LOG2E = 1.4426950408889634
F32 = jnp.float32
BF16 = jnp.bfloat16
MESH = pl.DeviceIdType.MESH
STATS = 128
GROUP = 8
PIECE = 256
LAG = 6
FLAG = 8
GU_BLOCK = 384
PAIR = 2
VMEM_LIMIT = 66_900_000


def dot(a, b):
    return jnp.dot(a, b, preferred_element_type=F32)


def attn_kernel(start_ref, hid_ref, freq_ref, norm_ref, qg_ref, kg_ref, wq_ref, wk_ref, wv_ref, kc_ref, vc_ref,
                o_ref, ko_ref, vo_ref,
                hid, normed, wq, wk, wv, kbuf, vbuf, cos, sin, raw, qs, ks, vs, ostage, thr, gain,
                hid_sem, w_sem, in_sem, out_sem, o_sem):
    n_rows, d_model = hid.shape
    n_batch, rows_kv, hd = kbuf.shape
    n_steps = n_rows // n_batch
    heads = wq.shape[1] // hd
    kv = wk.shape[1] // hd
    seq = rows_kv // kv
    n_groups = n_batch // GROUP
    qrows = heads * n_steps
    blk_start = lax.axis_index('sp') * seq

    hid_cp = pltpu.make_async_copy(hid_ref, hid, hid_sem)
    hid_cp.start()
    n_q = wq.shape[1] // 256
    w_cps = []
    for i in range(n_q):
        w_cps.append(pltpu.make_async_copy(wq_ref.at[:, pl.ds(i * 256, 256)], wq.at[:, pl.ds(i * 256, 256)], w_sem.at[i]))
    w_cps.append(pltpu.make_async_copy(wk_ref, wk, w_sem.at[n_q]))
    w_cps.append(pltpu.make_async_copy(wv_ref, wv, w_sem.at[n_q + 1]))
    w_cps[0].start()

    def cache_in(g, which):
        src, dst = ((kc_ref, kbuf), (vc_ref, vbuf))[which]
        rows = pl.ds(g * GROUP, GROUP)
        return pltpu.make_async_copy(src.at[rows], dst.at[rows], in_sem.at[which, g])

    def cache_out(g, which):
        src, dst = ((kbuf, ko_ref), (vbuf, vo_ref))[which]
        rows = pl.ds(g * GROUP, GROUP)
        return pltpu.make_async_copy(src.at[rows], dst.at[rows], out_sem.at[which, g])

    def o_out(g):
        rows = pl.ds(pl.multiple_of(g * GROUP * n_steps, GROUP * n_steps), GROUP * n_steps)
        return pltpu.make_async_copy(ostage.at[rows], o_ref.at[rows], o_sem.at[g])

    def start_in(g, c):
        cache_in(g, 0).start()
        cache_in(g, 1).start()
        return c

    ri = lax.broadcasted_iota(jnp.int32, (qrows, rows_kv), 0)
    ci = lax.broadcasted_iota(jnp.int32, (qrows, rows_kv), 1)
    row_kv = ri // (qrows // kv)
    thr[...] = jnp.where(ci % kv == row_kv, ci - kv * (ri % n_steps), 1 << 24)

    def set_pos(b, c):
        for i in range(n_steps):
            cos[pl.ds(b * n_steps + i, 1), :] = jnp.full((1, hd), start_ref[b] + i, jnp.int32).astype(F32)
        return c

    lax.fori_loop(0, n_batch, set_pos, 0)
    trows = 64
    low = lax.broadcasted_iota(jnp.int32, (trows, hd), 1) < hd // 2

    def table(i, c):
        rows = pl.ds(pl.multiple_of(i * trows, trows), trows)
        angle = cos[rows, :] * freq_ref[...]
        s = jnp.sin(angle)
        sin[rows, :] = jnp.where(low, -s, s)
        cos[rows, :] = jnp.cos(angle)
        return c

    lax.fori_loop(0, n_rows // trows, table, 0)

    for j in range(d_model // 128):
        gain[:, j * 128:(j + 1) * 128] = jnp.broadcast_to(norm_ref[j:j + 1, :].astype(F32), (8, 128))

    hid_cp.wait()
    for cp in w_cps[1:]:
        cp.start()
    chunk = 16

    def norm_rows(i, c):
        for u in range(4):
            rows = pl.ds(pl.multiple_of(i * 4 * chunk + u * chunk, chunk), chunk)
            sq = jnp.zeros((chunk, 128), F32)
            for j in range(d_model // 128):
                x = hid[rows, j * 128:(j + 1) * 128].astype(F32)
                sq = sq + x * x
            inv = lax.rsqrt(jnp.sum(sq, axis=-1, keepdims=True) * (1.0 / d_model) + NORM_EPS)
            for j in range(d_model // 128):
                sl = slice(j * 128, (j + 1) * 128)
                x = hid[rows, sl].astype(F32) * inv
                normed[rows, sl] = jnp.concatenate([x[:8] * gain[:, sl], x[8:] * gain[:, sl]], axis=0).astype(BF16)
        return c

    lax.fori_loop(0, n_rows // (4 * chunk), norm_rows, 0)

    pi = lax.broadcasted_iota(jnp.int32, (n_rows, n_rows), 0)
    pj = lax.broadcasted_iota(jnp.int32, (n_rows, n_rows), 1)
    perm = jnp.where(pj == (pi % n_steps) * n_batch + pi // n_steps, 1.0, 0.0).astype(BF16)
    for j in range(d_model // 256):
        sl = slice(j * 256, (j + 1) * 256)
        hid[:, sl] = dot(perm, normed[:, sl]).astype(BF16)

    def norm_rope(x, g, rows):
        inv = lax.rsqrt(jnp.mean(x * x, axis=-1, keepdims=True) + NORM_EPS)
        x = x * inv * g
        return (x * cos[rows, :] + pltpu.roll(x, hd // 2, 1) * sin[rows, :]).astype(BF16).astype(F32)

    qg = qg_ref[...].astype(F32)
    kg = kg_ref[...].astype(F32)

    def post(i):
        for r in range(n_rows // 64):
            rows = slice(r * 64, (r + 1) * 64)
            for h in range(2):
                x = raw[i % 2, rows, h * hd:(h + 1) * hd]
                if i < n_q:
                    qs[rows, i * 256 + h * hd:i * 256 + (h + 1) * hd] = norm_rope(x, qg, rows)
                elif i == n_q:
                    ks[pl.ds(r * 64 * kv + h, 64, stride=kv), :] = norm_rope(x, kg, rows)
                else:
                    vs[pl.ds(r * 64 * kv + h, 64, stride=kv), :] = x.astype(BF16).astype(F32)

    for i in range(n_q + 3):
        if i < n_q + 2:
            w_cps[i].wait()
            for g in range(n_groups * i // (n_q + 2), n_groups * (i + 1) // (n_q + 2)):
                start_in(g, 0)
            w = wq[:, i * 256:(i + 1) * 256] if i < n_q else (wk[...] if i == n_q else wv[...])
            for r in range(2):
                rr = slice(r * n_rows // 2, (r + 1) * n_rows // 2)
                raw[i % 2, rr] = dot(hid[rr], w)
        if i > 0:
            post(i - 1)

    scale = hd ** -0.5
    grows = GROUP * n_steps
    lane = lax.broadcasted_iota(jnp.int32, (grows, STATS), 1)
    win_rows = lax.broadcasted_iota(jnp.int32, (32, hd), 0)

    def group_step(g, c):
        cache_in(g, 0).wait()
        cache_in(g, 1).wait()
        rows = pl.ds(pl.multiple_of(g * grows, grows), grows)
        q_slab = qs[rows, :]
        offs = []
        for r in range(GROUP):
            b = g * GROUP + r
            off = kv * (start_ref[b] - blk_start)
            offs.append(off)
            win = pl.multiple_of(jnp.clip((off // 16) * 16, 0, rows_kv - 32), 16)
            n_new = n_steps * kv
            at = win_rows + (win - off)
            hit = jnp.logical_and(at >= 0, at < n_new)
            for buf, new_ref in ((kbuf, ks), (vbuf, vs)):
                new = pltpu.roll(new_ref[pl.ds(pl.multiple_of(b * n_new, n_new), n_new), :], off % n_new, 0)
                cur = buf[b, pl.ds(win, 32), :].astype(F32)
                cur = jnp.where(hit, jnp.concatenate([new] * (32 // n_new), axis=0), cur)
                buf[b, pl.ds(win, 32), :] = cur.astype(BF16)
        scores = []
        for r in range(GROUP):
            q = jnp.concatenate([q_slab[r * n_steps:(r + 1) * n_steps, h * hd:(h + 1) * hd] for h in range(heads)], axis=0)
            scores.append(lax.dot_general(q.astype(BF16), kbuf[g * GROUP + r], (((1,), (1,)), ((), ())),
                                          preferred_element_type=F32))
        probs, maxes, sums = [], [], []
        for r in range(GROUP):
            s = jnp.where(thr[...] <= offs[r] + kv - 1, scores[r], -jnp.inf)
            m = jnp.maximum(jnp.max(s, axis=-1, keepdims=True), LOWEST)
            p = jnp.exp2((s - m) * (scale * LOG2E))
            sums.append(jnp.sum(p, axis=-1, keepdims=True))
            maxes.append(m * scale)
            probs.append(p.astype(BF16))
        outs = [dot(probs[r], vbuf[g * GROUP + r]) for r in range(GROUP)]
        stats = jnp.zeros((grows, STATS), F32)
        for h in range(heads):
            sl = slice(h * n_steps, (h + 1) * n_steps)
            ostage[rows, h * hd:(h + 1) * hd] = jnp.concatenate([o[sl] for o in outs], axis=0)
            stats = jnp.where(lane == h, jnp.concatenate([m[sl] for m in maxes], axis=0), stats)
            stats = jnp.where(lane == heads + h, jnp.concatenate([t[sl] for t in sums], axis=0), stats)
        ostage[rows, heads * hd:] = stats
        cache_out(g, 0).start()
        cache_out(g, 1).start()
        o_out(g).start()
        return c

    lax.fori_loop(0, n_groups, group_step, 0)

    def drain(g, c):
        cache_out(g, 0).wait()
        cache_out(g, 1).wait()
        o_out(g).wait()
        return c

    lax.fori_loop(0, n_groups, drain, 0)


def attention(start_pos, hidden, freq, attn_norm, q_gain, k_gain, w_q, w_k, w_v, k_cache, v_cache):
    n_rows, d_model = hidden.shape
    n_batch, rows_kv, hd = k_cache.shape
    heads = w_q.shape[1] // hd
    n_groups = n_batch // GROUP
    n_steps = n_rows // n_batch
    n_w = w_q.shape[1] // 256 + 2
    width = heads * hd + STATS
    vmem = pl.BlockSpec(memory_space=pltpu.VMEM)
    hbm = pl.BlockSpec(memory_space=pl.ANY)
    return pl.pallas_call(
        attn_kernel,
        out_shape=(jax.ShapeDtypeStruct((n_rows, width), F32),
                   jax.ShapeDtypeStruct(k_cache.shape, BF16), jax.ShapeDtypeStruct(v_cache.shape, BF16)),
        in_specs=[pl.BlockSpec(memory_space=pltpu.SMEM), hbm, vmem, vmem, vmem, vmem, hbm, hbm, hbm, hbm, hbm],
        out_specs=(hbm, hbm, hbm),
        scratch_shapes=[
            pltpu.VMEM((n_rows, d_model), BF16), pltpu.VMEM((n_rows, d_model), BF16),
            pltpu.VMEM(w_q.shape, BF16), pltpu.VMEM(w_k.shape, BF16), pltpu.VMEM(w_v.shape, BF16),
            pltpu.VMEM(k_cache.shape, BF16), pltpu.VMEM(v_cache.shape, BF16),
            pltpu.VMEM((n_rows, hd), F32), pltpu.VMEM((n_rows, hd), F32), pltpu.VMEM((2, n_rows, 256), F32),
            pltpu.VMEM((n_rows, w_q.shape[1]), F32), pltpu.VMEM((n_rows * w_k.shape[1] // hd, hd), F32),
            pltpu.VMEM((n_rows * w_v.shape[1] // hd, hd), F32), pltpu.VMEM((n_rows, width), F32),
            pltpu.VMEM((heads * n_steps, rows_kv), jnp.int32), pltpu.VMEM((8, d_model), F32),
            pltpu.SemaphoreType.DMA, pltpu.SemaphoreType.DMA((n_w,)),
            pltpu.SemaphoreType.DMA((2, n_groups)), pltpu.SemaphoreType.DMA((2, n_groups)),
            pltpu.SemaphoreType.DMA((n_groups,)),
        ],
        compiler_params=pltpu.CompilerParams(vmem_limit_bytes=60_000_000),
        name="attn",
    )(start_pos, hidden, freq, attn_norm, q_gain, k_gain, w_q, w_k, w_v, k_cache, v_cache)


def mlp_kernel(o_ref, hid_ref, norm_ref, wo_ref, wg_ref, wu_ref, wd_ref,
               out_ref,
               x, wo, wg, wu, wd, loc, dbuf, ysend, yrecv, attn, pbuf, in_leaf, in_mid, tbuf, rbuf, mlp_in, act, fbuf, fy, fd,
               x_sem, w_sem, l_sem, d_ssem, d_rsem, y_ssem, y_rsem,
               up_s, up_r, mid_s, mid_r, dn_s, dn_r, fy_s, fy_r, fd_s, fd_r):
    me = lax.axis_index('sp')
    tp = lax.axis_index('tp')
    core = me % 2
    mate = me + 1 - 2 * core
    oth = (me + 2) % 4
    mate_oth = (mate + 2) % 4
    side = tp + 1 - 2 * (tp % 2)
    mid = 3 - tp
    inner = jnp.logical_or(tp == 1, tp == 2)
    leaf = jnp.logical_or(tp == 0, tp == 3)

    n_half, n_rows, d_model = x.shape
    n_pieces = d_model // PIECE
    width = loc.shape[2]
    hd = 128
    heads = (width - STATS) // hd
    n_chunks = dbuf.shape[1]
    crows = dbuf.shape[2]
    n_steps = out_ref.shape[0]
    n_req = n_rows // n_steps
    blk_req = n_req * n_half

    w_cps = [pltpu.make_async_copy(s, d, w_sem.at[i]) for i, (s, d) in
             enumerate(((wo_ref, wo), (wg_ref, wg), (wu_ref, wu), (wd_ref, wd)))]
    l_cps = [pltpu.make_async_copy(o_ref.at[oth], loc.at[0], l_sem.at[0]),
             pltpu.make_async_copy(o_ref.at[me], loc.at[1], l_sem.at[1])]
    x_cps = [pltpu.make_async_copy(
        hid_ref.at[i, pl.ds(pl.multiple_of(me * blk_req + h * n_req, n_req), n_req), :],
        x.at[h, pl.ds(i * n_req, n_req), :], x_sem.at[h, i]) for h in range(n_half) for i in range(n_steps)]
    for cp in l_cps:
        cp.start()

    barrier = pltpu.get_barrier_semaphore()
    for dev in ({'sp': mate}, {'sp': oth}, {'tp': side}):
        pl.semaphore_signal(barrier, inc=1, device_id=dev, device_id_type=MESH)

    @pl.when(inner)
    def _():
        pl.semaphore_signal(barrier, inc=1, device_id={'tp': mid}, device_id_type=MESH)
        pl.semaphore_wait(barrier, 4)

    @pl.when(leaf)
    def _():
        pl.semaphore_wait(barrier, 3)

    def remote(src, dst, ssem, rsem, dev):
        return pltpu.make_async_remote_copy(src_ref=src, dst_ref=dst, send_sem=ssem, recv_sem=rsem,
                                            device_id=dev, device_id_type=MESH)

    def d_copy(which, i):
        blk = (mate_oth, mate)[which]
        return remote(o_ref.at[blk, pl.ds(i * crows, crows), :], dbuf.at[which, i], d_ssem.at[which, i], d_rsem.at[which, i],
                      {'sp': mate})

    def y_copy(i):
        return remote(ysend.at[i], yrecv.at[i], y_ssem.at[i], y_rsem.at[i], {'sp': oth})

    for which in range(2):
        for i in range(n_chunks):
            d_copy(which, i).start()

    aw = heads * hd

    def weights(parts):
        m = functools.reduce(jnp.maximum, parts)
        es = [jnp.exp(s - m) for s in parts]
        tot = sum(e * pltpu.roll(s, STATS - heads, 1) for e, s in zip(es, parts))
        return m, es, tot

    stat_lane = lax.broadcasted_iota(jnp.int32, (crows, STATS), 1)
    l_cps[0].wait()
    for i in range(n_chunks):
        d_copy(0, i).wait_recv()
        rs = slice(i * crows, (i + 1) * crows)
        m, (ea, eb), tot = weights((loc[0, rs, aw:], dbuf[0, i, :, aw:]))
        for h in range(heads):
            sl = slice(h * hd, (h + 1) * hd)
            ysend[i, :, sl] = loc[0, rs, sl] * ea[:, h:h + 1] + dbuf[0, i, :, sl] * eb[:, h:h + 1]
        ysend[i, :, aw:] = jnp.where(stat_lane < heads, m, pltpu.roll(tot, heads, 1))
        y_copy(i).start()
        if i == 0:
            w_cps[0].start()
            for cp in x_cps:
                cp.start()
    l_cps[1].wait()
    for i in range(n_chunks):
        d_copy(1, i).wait_recv()
    for cp in w_cps[1:]:
        cp.start()

    pi = lax.broadcasted_iota(jnp.int32, (n_rows, n_rows), 0)
    pj = lax.broadcasted_iota(jnp.int32, (n_rows, n_rows), 1)
    perm = jnp.where(pj == (pi % n_req) * n_steps + pi // n_req, 1.0, 0.0).astype(BF16)

    def attn_half(hf):
        per = n_chunks // n_half
        for c in range(per):
            i = hf * per + c
            y_copy(i).wait_recv()
            rs = slice(i * crows, (i + 1) * crows)
            _, es, tot = weights((loc[1, rs, aw:], dbuf[1, i, :, aw:], yrecv[i, :, aw:]))
            inv = 1.0 / tot
            ea, eb, ec = [e * inv for e in es]
            for h in range(heads):
                sl = slice(h * hd, (h + 1) * hd)
                val = (loc[1, rs, sl] * ea[:, h:h + 1] + dbuf[1, i, :, sl] * eb[:, h:h + 1]
                       + yrecv[i, :, sl] * ec[:, h:h + 1])
                attn[hf, c * crows:(c + 1) * crows, sl] = val.astype(BF16)
        attn[hf] = dot(perm, attn[hf]).astype(BF16)

    def up(a, u):
        return remote(pbuf.at[a, u], in_leaf.at[a, u], up_s.at[a, u], up_r.at[a, u], {'tp': side})

    def across(a, u):
        return remote(pbuf.at[a, u], in_mid.at[a, u], mid_s.at[a, u], mid_r.at[a, u], {'tp': mid})

    def down(a, u):
        return remote(tbuf.at[a, u], tbuf.at[a, u], dn_s.at[a, u], dn_r.at[a, u], {'tp': side})

    def cols(k):
        if isinstance(k, int):
            return pl.ds(k * PIECE, PIECE)
        return pl.ds(pl.multiple_of(k * PIECE, PIECE), PIECE)

    def part(a, hf, k):
        left, right = ((attn, wo), (act, wd))[a]
        pbuf[a, hf * n_pieces + k] = dot(left[hf], right[:, cols(k)])

    def stage_a(a, u):
        up(a, u).wait_recv()
        pbuf[a, u] = pbuf[a, u] + in_leaf[a, u]
        across(a, u).start()

    def stage_b(a, u):
        across(a, u).wait_recv()
        tbuf[a, u] = pbuf[a, u] + in_mid[a, u]
        down(a, u).start()
        if a == 1:
            finish_out(u)

    def loop(lo, hi, body):
        def step(k, c):
            body(k)
            return c
        lax.fori_loop(lo, hi, step, 0)

    def parts(a, hf, sender=leaf):
        def body(i):
            for k in range(PAIR):
                part(a, hf, i * PAIR + k)

            @pl.when(sender)
            def _():
                for k in range(PAIR):
                    up(a, hf * n_pieces + i * PAIR + k).start()
        loop(0, n_pieces // PAIR, body)

    def norm_half(hf):
        base = hf * n_pieces

        @pl.when(leaf)
        def _():
            loop(0, n_pieces, lambda k: down(0, base + k).wait_recv())
        sq = jnp.zeros((n_rows, 128), F32)
        for k in range(n_pieces):
            r = (x[hf, :, cols(k)].astype(F32) + tbuf[0, base + k]).astype(BF16).astype(F32)
            rbuf[base + k] = r
            for j in range(PIECE // 128):
                piece = r[:, j * 128:(j + 1) * 128]
                sq = sq + piece * piece
        inv = lax.rsqrt(jnp.sum(sq, axis=-1, keepdims=True) * (1.0 / d_model) + NORM_EPS)
        for k in range(n_pieces):
            for j in range(PIECE // 128):
                c0 = k * PIECE + j * 128
                g = norm_ref[c0 // 128:c0 // 128 + 1, :].astype(F32)
                mlp_in[hf, :, c0:c0 + 128] = (rbuf[base + k, :, j * 128:(j + 1) * 128] * inv * g).astype(BF16)

    ffn = wg.shape[1]
    blocks = [(c, min(GU_BLOCK, ffn - c)) for c in range(0, ffn, GU_BLOCK)]
    def gate_up(hf, serve):
        for j, (c0, size) in enumerate(blocks):
            sl = slice(c0, c0 + size)
            gate = dot(mlp_in[hf], wg[:, sl])
            upv = dot(mlp_in[hf], wu[:, sl])
            act[hf, :, sl] = (gate * (1.0 / (1.0 + jnp.exp(-gate))) * upv).astype(BF16)

            @pl.when(inner)
            def _():
                serve(j)

    def put(blk, hf, k, val):
        val = val.astype(BF16)
        for i in range(n_steps):
            out_ref[i, pl.ds(pl.multiple_of(blk * blk_req + hf * n_req, n_req), n_req), cols(k)] = val[i * n_req:(i + 1) * n_req]

    def f_y(u):
        return remote(fbuf.at[u], fy.at[u], fy_s.at[u], fy_r.at[u], {'sp': oth})

    def f_d(which, u):
        src = (fbuf, fy)[which]
        return remote(src.at[u], fd.at[which, u], fd_s.at[which, u], fd_r.at[which, u], {'sp': mate})

    def forward(u):
        f_y(u).wait_recv()
        f_d(1, u).start()
        put(oth, u // n_pieces, u % n_pieces, fy[u])

    def finish_out(u):
        val = (rbuf[u] + tbuf[1, u]).astype(BF16)
        fbuf[u] = val.astype(F32)
        f_y(u).start()
        f_d(0, u).start()
        put(me, u // n_pieces, u % n_pieces, val)
        if isinstance(u, int):
            if u >= FLAG:
                forward(u - FLAG)
        else:
            @pl.when(u >= FLAG)
            def _():
                forward(u - FLAG)

    w_cps[0].wait()
    attn_half(0)
    parts(0, 0, jnp.logical_and(leaf, core == 0))
    attn_half(1)

    @pl.when(jnp.logical_and(leaf, core == 1))
    def _():
        loop(0, n_pieces, lambda u: up(0, u).start())
    n_u = n_half * n_pieces

    @pl.when(leaf)
    def _():
        parts(0, 1)

    @pl.when(inner)
    def _():
        def head(u):
            part(0, 1, u)
            stage_a(0, u)
        loop(0, LAG, head)

        def body(u):
            head(u)
            stage_b(0, u - LAG)
        loop(LAG, n_pieces, body)

        def rest(u):
            stage_a(0, u)
            stage_b(0, u - LAG)
        loop(n_pieces, n_u, rest)

    for cp in x_cps:
        cp.wait()
    norm_half(0)
    w_cps[1].wait()
    w_cps[2].wait()

    def serve0(j):
        if j < LAG:
            stage_b(0, n_u - LAG + j)
    gate_up(0, serve0)
    w_cps[3].wait()

    parts(1, 0)
    norm_half(1)
    shares = [[int(u) for u in s] for s in np.array_split(np.arange(n_pieces), len(blocks))]

    def serve1(j):
        for u in shares[j]:
            stage_a(1, u)
            if u >= LAG:
                stage_b(1, u - LAG)
    gate_up(1, serve1)
    parts(1, 1)

    @pl.when(leaf)
    def _():
        def take(u):
            down(1, u).wait_recv()
            finish_out(u)
        loop(0, n_u, take)

    @pl.when(inner)
    def _():
        loop(n_pieces - LAG, n_pieces, lambda u: stage_b(1, u))
        loop(n_pieces, n_pieces + LAG, lambda u: stage_a(1, u))

        def body(u):
            stage_a(1, u)
            stage_b(1, u - LAG)
        loop(n_pieces + LAG, n_u, body)
        loop(n_u - LAG, n_u, lambda u: stage_b(1, u))

    loop(2 * n_pieces - FLAG, 2 * n_pieces, forward)

    for hf in range(n_half):
        def last(k, hf=hf):
            u = hf * n_pieces + k
            f_d(0, u).wait_recv()
            put(mate, hf, k, fd[0, u])
            f_d(1, u).wait_recv()
            put(mate_oth, hf, k, fd[1, u])
        loop(0, n_pieces, last)

    for which in range(2):
        for i in range(n_chunks):
            d_copy(which, i).wait_send()
    for i in range(n_chunks):
        y_copy(i).wait_send()

    def sends(u):
        f_y(u).wait_send()
        f_d(0, u).wait_send()
        f_d(1, u).wait_send()
        for a in range(2):
            @pl.when(leaf)
            def _():
                up(a, u).wait_send()

            @pl.when(inner)
            def _():
                across(a, u).wait_send()
                down(a, u).wait_send()
    loop(0, n_half * n_pieces, sends)


def mlp(o_part, hidden, mlp_norm, w_o, w_gate, w_up, w_down):
    n_blk, blk_rows, width = o_part.shape
    n_steps, n_batch, d_model = hidden.shape
    n_half = 2
    n_rows = blk_rows // n_half
    n_pieces = d_model // PIECE
    n_chunks = 4
    crows = blk_rows // n_chunks
    ffn = w_gate.shape[1]
    vmem = pl.BlockSpec(memory_space=pltpu.VMEM)
    hbm = pl.BlockSpec(memory_space=pl.ANY)
    dma = pltpu.SemaphoreType.DMA
    n_u = n_half * n_pieces
    piece = (n_u, n_rows, PIECE)
    return pl.pallas_call(
        mlp_kernel,
        out_shape=jax.ShapeDtypeStruct(hidden.shape, BF16),
        in_specs=[hbm, hbm, vmem, hbm, hbm, hbm, hbm],
        out_specs=vmem,
        scratch_shapes=[
            pltpu.VMEM((n_half, n_rows, d_model), BF16),
            pltpu.VMEM(w_o.shape, BF16), pltpu.VMEM(w_gate.shape, BF16),
            pltpu.VMEM(w_up.shape, BF16), pltpu.VMEM(w_down.shape, BF16),
            pltpu.VMEM((2, blk_rows, width), F32), pltpu.VMEM((2, n_chunks, crows, width), F32),
            pltpu.VMEM((n_chunks, crows, width), F32), pltpu.VMEM((n_chunks, crows, width), F32),
            pltpu.VMEM((n_half, n_rows, w_o.shape[0]), BF16),
            pltpu.VMEM((2,) + piece, F32), pltpu.VMEM((2,) + piece, F32),
            pltpu.VMEM((2,) + piece, F32), pltpu.VMEM((2,) + piece, F32),
            pltpu.VMEM(piece, F32), pltpu.VMEM((n_half, n_rows, d_model), BF16), pltpu.VMEM((n_half, n_rows, ffn), BF16),
            pltpu.VMEM(piece, F32), pltpu.VMEM(piece, F32), pltpu.VMEM((2,) + piece, F32),
            dma((n_half, n_steps)), dma((4,)), dma((2,)),
            dma((2, n_chunks)), dma((2, n_chunks)), dma((n_chunks,)), dma((n_chunks,)),
            dma((2, n_u)), dma((2, n_u)), dma((2, n_u)), dma((2, n_u)), dma((2, n_u)), dma((2, n_u)),
            dma((n_u,)), dma((n_u,)), dma((2, n_u)), dma((2, n_u)),
        ],
        compiler_params=pltpu.CompilerParams(vmem_limit_bytes=VMEM_LIMIT, collective_id=0, has_side_effects=True),
        name="combine_mlp",
    )(o_part, hidden, mlp_norm, w_o, w_gate, w_up, w_down)


def solution(mesh):
    cache_spec = P('dp', 'sp', 'tp', None)
    col_spec = P(None, 'tp')
    row_spec = P('tp', None)
    in_specs = (P(None, 'dp', None), P('dp'), cache_spec, cache_spec, col_spec, col_spec, col_spec, row_spec,
                col_spec, col_spec, row_spec, P(), P(), P(), P())
    out_specs = (P(None, 'dp', None), cache_spec, cache_spec)

    def shard_body(hidden, start_pos, k_cache, v_cache, w_q, w_k, w_v, w_o, w_gate, w_up, w_down, attn_norm, mlp_norm, q_gain, k_gain):
        n_steps, n_batch, d_model = hidden.shape
        _, seq, kv, hd = k_cache.shape
        half = np.arange(hd // 2)
        freq = ROPE_BASE ** (-half * (2.0 / hd))
        freq = jnp.asarray(np.concatenate([freq, freq])[None], F32)
        o_part, k_out, v_out = attention(
            start_pos, hidden.reshape(-1, d_model), freq, attn_norm.reshape(-1, 128), q_gain[None], k_gain[None],
            w_q, w_k, w_v, k_cache.reshape(n_batch, seq * kv, hd), v_cache.reshape(n_batch, seq * kv, hd))
        n_sp = 4
        out = mlp(o_part.reshape(n_sp, -1, o_part.shape[1]), hidden, mlp_norm.reshape(-1, 128), w_o, w_gate, w_up, w_down)
        return out, k_out.reshape(k_cache.shape), v_out.reshape(v_cache.shape)

    return jax.shard_map(shard_body, mesh=mesh, in_specs=in_specs, out_specs=out_specs, check_vma=False)
```

```python
import functools
import jax
import jax.numpy as jnp
import numpy as np
from jax import lax
from jax.experimental import pallas as pl
from jax.experimental.pallas import tpu as pltpu
from jax.sharding import PartitionSpec as P

ROPE_BASE = 1000000.0
NORM_EPS = 1e-06
LOWEST = float(np.finfo(np.float32).min)
LOG2E = 1.4426950408889634
F32 = jnp.float32
BF16 = jnp.bfloat16
MESH = pl.DeviceIdType.MESH
STATS = 128
GROUP = 16
PIECE = 512
LAG = 3
FLAG = 5
GU_BLOCK = 384
PAIR = 1
VMEM_LIMIT = 66_900_000


def dot(a, b):
    return jnp.dot(a, b, preferred_element_type=F32)


def attn_kernel(start_ref, hid_ref, freq_ref, norm_ref, qg_ref, kg_ref, wq_ref, wk_ref, wv_ref, kc_ref, vc_ref,
                o_ref, ko_ref, vo_ref,
                hid, normed, wq, wk, wv, kbuf, vbuf, cos, sin, raw, qs, ks, vs, ostage, thr, gain,
                hid_sem, w_sem, in_sem, out_sem, o_sem):
    n_rows, d_model = hid.shape
    n_batch, rows_kv, hd = kbuf.shape
    n_steps = n_rows // n_batch
    heads = wq.shape[1] // hd
    kv = wk.shape[1] // hd
    seq = rows_kv // kv
    n_groups = n_batch // GROUP
    qrows = heads * n_steps
    blk_start = lax.axis_index('sp') * seq

    hid_cp = pltpu.make_async_copy(hid_ref, hid, hid_sem)
    hid_cp.start()
    n_q = wq.shape[1] // 256
    w_cps = []
    for i in range(n_q):
        w_cps.append(pltpu.make_async_copy(wq_ref.at[:, pl.ds(i * 256, 256)], wq.at[:, pl.ds(i * 256, 256)], w_sem.at[i]))
    w_cps.append(pltpu.make_async_copy(wk_ref, wk, w_sem.at[n_q]))
    w_cps.append(pltpu.make_async_copy(wv_ref, wv, w_sem.at[n_q + 1]))
    w_cps[0].start()

    def cache_in(g, which):
        src, dst = ((kc_ref, kbuf), (vc_ref, vbuf))[which]
        rows = pl.ds(g * GROUP, GROUP)
        return pltpu.make_async_copy(src.at[rows], dst.at[rows], in_sem.at[which, g])

    def cache_out(g, which):
        src, dst = ((kbuf, ko_ref), (vbuf, vo_ref))[which]
        rows = pl.ds(g * GROUP, GROUP)
        return pltpu.make_async_copy(src.at[rows], dst.at[rows], out_sem.at[which, g])

    def o_out(g):
        rows = pl.ds(pl.multiple_of(g * GROUP * n_steps, GROUP * n_steps), GROUP * n_steps)
        return pltpu.make_async_copy(ostage.at[rows], o_ref.at[rows], o_sem.at[g])

    def start_in(g, c):
        cache_in(g, 0).start()
        cache_in(g, 1).start()
        return c

    ri = lax.broadcasted_iota(jnp.int32, (qrows, rows_kv), 0)
    ci = lax.broadcasted_iota(jnp.int32, (qrows, rows_kv), 1)
    row_kv = ri // (qrows // kv)
    thr[...] = jnp.where(ci % kv == row_kv, ci - kv * (ri % n_steps), 1 << 24)

    def set_pos(b, c):
        for i in range(n_steps):
            cos[pl.ds(b * n_steps + i, 1), :] = jnp.full((1, hd), start_ref[b] + i, jnp.int32).astype(F32)
        return c

    lax.fori_loop(0, n_batch, set_pos, 0)
    trows = 64
    low = lax.broadcasted_iota(jnp.int32, (trows, hd), 1) < hd // 2

    def table(i, c):
        rows = pl.ds(pl.multiple_of(i * trows, trows), trows)
        angle = cos[rows, :] * freq_ref[...]
        s = jnp.sin(angle)
        sin[rows, :] = jnp.where(low, -s, s)
        cos[rows, :] = jnp.cos(angle)
        return c

    lax.fori_loop(0, n_rows // trows, table, 0)

    for j in range(d_model // 128):
        gain[:, j * 128:(j + 1) * 128] = jnp.broadcast_to(norm_ref[j:j + 1, :].astype(F32), (8, 128))

    hid_cp.wait()
    for cp in w_cps[1:]:
        cp.start()
    chunk = 16

    def norm_rows(i, c):
        for u in range(4):
            rows = pl.ds(pl.multiple_of(i * 4 * chunk + u * chunk, chunk), chunk)
            sq = jnp.zeros((chunk, 128), F32)
            for j in range(d_model // 128):
                x = hid[rows, j * 128:(j + 1) * 128].astype(F32)
                sq = sq + x * x
            inv = lax.rsqrt(jnp.sum(sq, axis=-1, keepdims=True) * (1.0 / d_model) + NORM_EPS)
            for j in range(d_model // 128):
                sl = slice(j * 128, (j + 1) * 128)
                x = hid[rows, sl].astype(F32) * inv
                normed[rows, sl] = jnp.concatenate([x[:8] * gain[:, sl], x[8:] * gain[:, sl]], axis=0).astype(BF16)
        return c

    lax.fori_loop(0, n_rows // (4 * chunk), norm_rows, 0)

    pi = lax.broadcasted_iota(jnp.int32, (n_rows, n_rows), 0)
    pj = lax.broadcasted_iota(jnp.int32, (n_rows, n_rows), 1)
    perm = jnp.where(pj == (pi % n_steps) * n_batch + pi // n_steps, 1.0, 0.0).astype(BF16)
    for j in range(d_model // 256):
        sl = slice(j * 256, (j + 1) * 256)
        hid[:, sl] = dot(perm, normed[:, sl]).astype(BF16)

    def norm_rope(x, g, rows):
        inv = lax.rsqrt(jnp.mean(x * x, axis=-1, keepdims=True) + NORM_EPS)
        x = x * inv * g
        return (x * cos[rows, :] + pltpu.roll(x, hd // 2, 1) * sin[rows, :]).astype(BF16).astype(F32)

    qg = qg_ref[...].astype(F32)
    kg = kg_ref[...].astype(F32)

    def post(i):
        for r in range(n_rows // 64):
            rows = slice(r * 64, (r + 1) * 64)
            for h in range(2):
                x = raw[i % 2, rows, h * hd:(h + 1) * hd]
                if i < n_q:
                    qs[rows, i * 256 + h * hd:i * 256 + (h + 1) * hd] = norm_rope(x, qg, rows)
                elif i == n_q:
                    ks[pl.ds(r * 64 * kv + h, 64, stride=kv), :] = norm_rope(x, kg, rows)
                else:
                    vs[pl.ds(r * 64 * kv + h, 64, stride=kv), :] = x.astype(BF16).astype(F32)

    for i in range(n_q + 3):
        if i < n_q + 2:
            w_cps[i].wait()
            for g in range(n_groups * i // (n_q + 2), n_groups * (i + 1) // (n_q + 2)):
                start_in(g, 0)
            w = wq[:, i * 256:(i + 1) * 256] if i < n_q else (wk[...] if i == n_q else wv[...])
            for r in range(2):
                rr = slice(r * n_rows // 2, (r + 1) * n_rows // 2)
                raw[i % 2, rr] = dot(hid[rr], w)
        if i > 0:
            post(i - 1)

    scale = hd ** -0.5
    grows = GROUP * n_steps
    lane = lax.broadcasted_iota(jnp.int32, (grows, STATS), 1)
    win_rows = lax.broadcasted_iota(jnp.int32, (32, hd), 0)

    def group_step(g, c):
        cache_in(g, 0).wait()
        cache_in(g, 1).wait()
        rows = pl.ds(pl.multiple_of(g * grows, grows), grows)
        q_slab = qs[rows, :]
        offs = []
        for r in range(GROUP):
            b = g * GROUP + r
            off = kv * (start_ref[b] - blk_start)
            offs.append(off)
            win = pl.multiple_of(jnp.clip((off // 16) * 16, 0, rows_kv - 32), 16)
            n_new = n_steps * kv
            at = win_rows + (win - off)
            hit = jnp.logical_and(at >= 0, at < n_new)
            for buf, new_ref in ((kbuf, ks), (vbuf, vs)):
                new = pltpu.roll(new_ref[pl.ds(pl.multiple_of(b * n_new, n_new), n_new), :], off % n_new, 0)
                cur = buf[b, pl.ds(win, 32), :].astype(F32)
                cur = jnp.where(hit, jnp.concatenate([new] * (32 // n_new), axis=0), cur)
                buf[b, pl.ds(win, 32), :] = cur.astype(BF16)
        scores = []
        for r in range(GROUP):
            q = jnp.concatenate([q_slab[r * n_steps:(r + 1) * n_steps, h * hd:(h + 1) * hd] for h in range(heads)], axis=0)
            scores.append(lax.dot_general(q.astype(BF16), kbuf[g * GROUP + r], (((1,), (1,)), ((), ())),
                                          preferred_element_type=F32))
        probs, maxes, sums = [], [], []
        for r in range(GROUP):
            s = jnp.where(thr[...] <= offs[r] + kv - 1, scores[r], -jnp.inf)
            m = jnp.maximum(jnp.max(s, axis=-1, keepdims=True), LOWEST)
            p = jnp.exp2((s - m) * (scale * LOG2E))
            sums.append(jnp.sum(p, axis=-1, keepdims=True))
            maxes.append(m * scale)
            probs.append(p.astype(BF16))
        outs = [dot(probs[r], vbuf[g * GROUP + r]) for r in range(GROUP)]
        stats = jnp.zeros((grows, STATS), F32)
        for h in range(heads):
            sl = slice(h * n_steps, (h + 1) * n_steps)
            ostage[rows, h * hd:(h + 1) * hd] = jnp.concatenate([o[sl] for o in outs], axis=0)
            stats = jnp.where(lane == h, jnp.concatenate([m[sl] for m in maxes], axis=0), stats)
            stats = jnp.where(lane == heads + h, jnp.concatenate([t[sl] for t in sums], axis=0), stats)
        ostage[rows, heads * hd:] = stats
        cache_out(g, 0).start()
        cache_out(g, 1).start()
        o_out(g).start()
        return c

    lax.fori_loop(0, n_groups, group_step, 0)

    def drain(g, c):
        cache_out(g, 0).wait()
        cache_out(g, 1).wait()
        o_out(g).wait()
        return c

    lax.fori_loop(0, n_groups, drain, 0)


def attention(start_pos, hidden, freq, attn_norm, q_gain, k_gain, w_q, w_k, w_v, k_cache, v_cache):
    n_rows, d_model = hidden.shape
    n_batch, rows_kv, hd = k_cache.shape
    heads = w_q.shape[1] // hd
    n_groups = n_batch // GROUP
    n_steps = n_rows // n_batch
    n_w = w_q.shape[1] // 256 + 2
    width = heads * hd + STATS
    vmem = pl.BlockSpec(memory_space=pltpu.VMEM)
    hbm = pl.BlockSpec(memory_space=pl.ANY)
    return pl.pallas_call(
        attn_kernel,
        out_shape=(jax.ShapeDtypeStruct((n_rows, width), F32),
                   jax.ShapeDtypeStruct(k_cache.shape, BF16), jax.ShapeDtypeStruct(v_cache.shape, BF16)),
        in_specs=[pl.BlockSpec(memory_space=pltpu.SMEM), hbm, vmem, vmem, vmem, vmem, hbm, hbm, hbm, hbm, hbm],
        out_specs=(hbm, hbm, hbm),
        scratch_shapes=[
            pltpu.VMEM((n_rows, d_model), BF16), pltpu.VMEM((n_rows, d_model), BF16),
            pltpu.VMEM(w_q.shape, BF16), pltpu.VMEM(w_k.shape, BF16), pltpu.VMEM(w_v.shape, BF16),
            pltpu.VMEM(k_cache.shape, BF16), pltpu.VMEM(v_cache.shape, BF16),
            pltpu.VMEM((n_rows, hd), F32), pltpu.VMEM((n_rows, hd), F32), pltpu.VMEM((2, n_rows, 256), F32),
            pltpu.VMEM((n_rows, w_q.shape[1]), F32), pltpu.VMEM((n_rows * w_k.shape[1] // hd, hd), F32),
            pltpu.VMEM((n_rows * w_v.shape[1] // hd, hd), F32), pltpu.VMEM((n_rows, width), F32),
            pltpu.VMEM((heads * n_steps, rows_kv), jnp.int32), pltpu.VMEM((8, d_model), F32),
            pltpu.SemaphoreType.DMA, pltpu.SemaphoreType.DMA((n_w,)),
            pltpu.SemaphoreType.DMA((2, n_groups)), pltpu.SemaphoreType.DMA((2, n_groups)),
            pltpu.SemaphoreType.DMA((n_groups,)),
        ],
        compiler_params=pltpu.CompilerParams(vmem_limit_bytes=60_000_000),
        name="attn",
    )(start_pos, hidden, freq, attn_norm, q_gain, k_gain, w_q, w_k, w_v, k_cache, v_cache)


def mlp_kernel(o_ref, hid_ref, norm_ref, wo_ref, wg_ref, wu_ref, wd_ref,
               out_ref,
               x, wo, wg, wu, wd, loc, dbuf, ysend, yrecv, attn, pbuf, in_leaf, in_mid, tbuf, rbuf, mlp_in, act, fbuf, fy, fd,
               x_sem, w_sem, l_sem, d_ssem, d_rsem, y_ssem, y_rsem,
               up_s, up_r, mid_s, mid_r, dn_s, dn_r, fy_s, fy_r, fd_s, fd_r):
    me = lax.axis_index('sp')
    tp = lax.axis_index('tp')
    core = me % 2
    mate = me + 1 - 2 * core
    oth = (me + 2) % 4
    mate_oth = (mate + 2) % 4
    side = tp + 1 - 2 * (tp % 2)
    mid = 3 - tp
    inner = jnp.logical_or(tp == 1, tp == 2)
    leaf = jnp.logical_or(tp == 0, tp == 3)

    n_half, n_rows, d_model = x.shape
    n_pieces = d_model // PIECE
    width = loc.shape[2]
    hd = 128
    heads = (width - STATS) // hd
    n_chunks = dbuf.shape[1]
    crows = dbuf.shape[2]
    n_steps = out_ref.shape[0]
    n_req = n_rows // n_steps
    blk_req = n_req * n_half

    w_cps = [pltpu.make_async_copy(s, d, w_sem.at[i]) for i, (s, d) in
             enumerate(((wo_ref, wo), (wg_ref, wg), (wu_ref, wu), (wd_ref, wd)))]
    l_cps = [pltpu.make_async_copy(o_ref.at[oth], loc.at[0], l_sem.at[0]),
             pltpu.make_async_copy(o_ref.at[me], loc.at[1], l_sem.at[1])]
    x_cps = [pltpu.make_async_copy(
        hid_ref.at[i, pl.ds(pl.multiple_of(me * blk_req + h * n_req, n_req), n_req), :],
        x.at[h, pl.ds(i * n_req, n_req), :], x_sem.at[h, i]) for h in range(n_half) for i in range(n_steps)]
    for cp in l_cps:
        cp.start()

    barrier = pltpu.get_barrier_semaphore()
    for dev in ({'sp': mate}, {'sp': oth}, {'tp': side}):
        pl.semaphore_signal(barrier, inc=1, device_id=dev, device_id_type=MESH)

    @pl.when(inner)
    def _():
        pl.semaphore_signal(barrier, inc=1, device_id={'tp': mid}, device_id_type=MESH)
        pl.semaphore_wait(barrier, 4)

    @pl.when(leaf)
    def _():
        pl.semaphore_wait(barrier, 3)

    def remote(src, dst, ssem, rsem, dev):
        return pltpu.make_async_remote_copy(src_ref=src, dst_ref=dst, send_sem=ssem, recv_sem=rsem,
                                            device_id=dev, device_id_type=MESH)

    def d_copy(which, i):
        blk = (mate_oth, mate)[which]
        return remote(o_ref.at[blk, pl.ds(i * crows, crows), :], dbuf.at[which, i], d_ssem.at[which, i], d_rsem.at[which, i],
                      {'sp': mate})

    def y_copy(i):
        return remote(ysend.at[i], yrecv.at[i], y_ssem.at[i], y_rsem.at[i], {'sp': oth})

    for which in range(2):
        for i in range(n_chunks):
            d_copy(which, i).start()

    aw = heads * hd

    def weights(parts):
        m = functools.reduce(jnp.maximum, parts)
        es = [jnp.exp(s - m) for s in parts]
        tot = sum(e * pltpu.roll(s, STATS - heads, 1) for e, s in zip(es, parts))
        return m, es, tot

    stat_lane = lax.broadcasted_iota(jnp.int32, (crows, STATS), 1)
    l_cps[0].wait()
    for i in range(n_chunks):
        d_copy(0, i).wait_recv()
        rs = slice(i * crows, (i + 1) * crows)
        m, (ea, eb), tot = weights((loc[0, rs, aw:], dbuf[0, i, :, aw:]))
        for h in range(heads):
            sl = slice(h * hd, (h + 1) * hd)
            ysend[i, :, sl] = loc[0, rs, sl] * ea[:, h:h + 1] + dbuf[0, i, :, sl] * eb[:, h:h + 1]
        ysend[i, :, aw:] = jnp.where(stat_lane < heads, m, pltpu.roll(tot, heads, 1))
        y_copy(i).start()
        if i == 0:
            w_cps[0].start()
            for cp in x_cps:
                cp.start()
    l_cps[1].wait()
    for i in range(n_chunks):
        d_copy(1, i).wait_recv()
    for cp in w_cps[1:]:
        cp.start()

    pi = lax.broadcasted_iota(jnp.int32, (n_rows, n_rows), 0)
    pj = lax.broadcasted_iota(jnp.int32, (n_rows, n_rows), 1)
    perm = jnp.where(pj == (pi % n_req) * n_steps + pi // n_req, 1.0, 0.0).astype(BF16)

    def attn_half(hf):
        per = n_chunks // n_half
        for c in range(per):
            i = hf * per + c
            y_copy(i).wait_recv()
            rs = slice(i * crows, (i + 1) * crows)
            _, es, tot = weights((loc[1, rs, aw:], dbuf[1, i, :, aw:], yrecv[i, :, aw:]))
            inv = 1.0 / tot
            ea, eb, ec = [e * inv for e in es]
            for h in range(heads):
                sl = slice(h * hd, (h + 1) * hd)
                val = (loc[1, rs, sl] * ea[:, h:h + 1] + dbuf[1, i, :, sl] * eb[:, h:h + 1]
                       + yrecv[i, :, sl] * ec[:, h:h + 1])
                attn[hf, c * crows:(c + 1) * crows, sl] = val.astype(BF16)
        attn[hf] = dot(perm, attn[hf]).astype(BF16)

    def up(a, u):
        return remote(pbuf.at[a, u], in_leaf.at[a, u], up_s.at[a, u], up_r.at[a, u], {'tp': side})

    def across(a, u):
        return remote(pbuf.at[a, u], in_mid.at[a, u], mid_s.at[a, u], mid_r.at[a, u], {'tp': mid})

    def down(a, u):
        return remote(tbuf.at[a, u], tbuf.at[a, u], dn_s.at[a, u], dn_r.at[a, u], {'tp': side})

    def cols(k):
        if isinstance(k, int):
            return pl.ds(k * PIECE, PIECE)
        return pl.ds(pl.multiple_of(k * PIECE, PIECE), PIECE)

    def part(a, hf, k):
        left, right = ((attn, wo), (act, wd))[a]
        pbuf[a, hf * n_pieces + k] = dot(left[hf], right[:, cols(k)])

    def stage_a(a, u):
        up(a, u).wait_recv()
        pbuf[a, u] = pbuf[a, u] + in_leaf[a, u]
        across(a, u).start()

    def stage_b(a, u):
        across(a, u).wait_recv()
        tbuf[a, u] = pbuf[a, u] + in_mid[a, u]
        down(a, u).start()
        if a == 1:
            finish_out(u)

    def loop(lo, hi, body):
        def step(k, c):
            body(k)
            return c
        lax.fori_loop(lo, hi, step, 0)

    def parts(a, hf, sender=leaf):
        def body(i):
            for k in range(PAIR):
                part(a, hf, i * PAIR + k)

            @pl.when(sender)
            def _():
                for k in range(PAIR):
                    up(a, hf * n_pieces + i * PAIR + k).start()
        loop(0, n_pieces // PAIR, body)

    def norm_half(hf):
        base = hf * n_pieces

        @pl.when(leaf)
        def _():
            loop(0, n_pieces, lambda k: down(0, base + k).wait_recv())
        sq = jnp.zeros((n_rows, 128), F32)
        for k in range(n_pieces):
            r = (x[hf, :, cols(k)].astype(F32) + tbuf[0, base + k]).astype(BF16).astype(F32)
            rbuf[base + k] = r
            for j in range(PIECE // 128):
                piece = r[:, j * 128:(j + 1) * 128]
                sq = sq + piece * piece
        inv = lax.rsqrt(jnp.sum(sq, axis=-1, keepdims=True) * (1.0 / d_model) + NORM_EPS)
        for k in range(n_pieces):
            for j in range(PIECE // 128):
                c0 = k * PIECE + j * 128
                g = norm_ref[c0 // 128:c0 // 128 + 1, :].astype(F32)
                mlp_in[hf, :, c0:c0 + 128] = (rbuf[base + k, :, j * 128:(j + 1) * 128] * inv * g).astype(BF16)

    ffn = wg.shape[1]
    blocks = [(c, min(GU_BLOCK, ffn - c)) for c in range(0, ffn, GU_BLOCK)]
    def gate_up(hf, serve):
        for j, (c0, size) in enumerate(blocks):
            sl = slice(c0, c0 + size)
            gate = dot(mlp_in[hf], wg[:, sl])
            upv = dot(mlp_in[hf], wu[:, sl])
            act[hf, :, sl] = (gate * (1.0 / (1.0 + jnp.exp(-gate))) * upv).astype(BF16)

            @pl.when(inner)
            def _():
                serve(j)

    def put(blk, hf, k, val):
        val = val.astype(BF16)
        for i in range(n_steps):
            out_ref[i, pl.ds(pl.multiple_of(blk * blk_req + hf * n_req, n_req), n_req), cols(k)] = val[i * n_req:(i + 1) * n_req]

    def f_y(u):
        return remote(fbuf.at[u], fy.at[u], fy_s.at[u], fy_r.at[u], {'sp': oth})

    def f_d(which, u):
        src = (fbuf, fy)[which]
        return remote(src.at[u], fd.at[which, u], fd_s.at[which, u], fd_r.at[which, u], {'sp': mate})

    def forward(u):
        f_y(u).wait_recv()
        f_d(1, u).start()
        put(oth, u // n_pieces, u % n_pieces, fy[u])

    def finish_out(u):
        val = (rbuf[u] + tbuf[1, u]).astype(BF16)
        fbuf[u] = val.astype(F32)
        f_y(u).start()
        f_d(0, u).start()
        put(me, u // n_pieces, u % n_pieces, val)
        if isinstance(u, int):
            if u >= FLAG:
                forward(u - FLAG)
        else:
            @pl.when(u >= FLAG)
            def _():
                forward(u - FLAG)

    w_cps[0].wait()
    attn_half(0)
    parts(0, 0, jnp.logical_and(leaf, core == 0))
    attn_half(1)

    @pl.when(jnp.logical_and(leaf, core == 1))
    def _():
        loop(0, n_pieces, lambda u: up(0, u).start())
    n_u = n_half * n_pieces

    @pl.when(leaf)
    def _():
        parts(0, 1)

    @pl.when(inner)
    def _():
        def head(u):
            part(0, 1, u)
            stage_a(0, u)
        loop(0, LAG, head)

        def body(u):
            head(u)
            stage_b(0, u - LAG)
        loop(LAG, n_pieces, body)

        def rest(u):
            stage_a(0, u)
            stage_b(0, u - LAG)
        loop(n_pieces, n_u, rest)

    for cp in x_cps:
        cp.wait()
    norm_half(0)
    w_cps[1].wait()
    w_cps[2].wait()

    def serve0(j):
        if j < LAG:
            stage_b(0, n_u - LAG + j)
    gate_up(0, serve0)
    w_cps[3].wait()

    parts(1, 0)
    norm_half(1)
    shares = [[int(u) for u in s] for s in np.array_split(np.arange(n_pieces), len(blocks))]

    def serve1(j):
        for u in shares[j]:
            stage_a(1, u)
            if u >= LAG:
                stage_b(1, u - LAG)
    gate_up(1, serve1)
    parts(1, 1)

    @pl.when(leaf)
    def _():
        def take(u):
            down(1, u).wait_recv()
            finish_out(u)
        loop(0, n_u, take)

    @pl.when(inner)
    def _():
        loop(n_pieces - LAG, n_pieces, lambda u: stage_b(1, u))
        loop(n_pieces, n_pieces + LAG, lambda u: stage_a(1, u))

        def body(u):
            stage_a(1, u)
            stage_b(1, u - LAG)
        loop(n_pieces + LAG, n_u, body)
        loop(n_u - LAG, n_u, lambda u: stage_b(1, u))

    loop(2 * n_pieces - FLAG, 2 * n_pieces, forward)

    for hf in range(n_half):
        def last(k, hf=hf):
            u = hf * n_pieces + k
            f_d(0, u).wait_recv()
            put(mate, hf, k, fd[0, u])
            f_d(1, u).wait_recv()
            put(mate_oth, hf, k, fd[1, u])
        loop(0, n_pieces, last)

    for which in range(2):
        for i in range(n_chunks):
            d_copy(which, i).wait_send()
    for i in range(n_chunks):
        y_copy(i).wait_send()

    def sends(u):
        f_y(u).wait_send()
        f_d(0, u).wait_send()
        f_d(1, u).wait_send()
        for a in range(2):
            @pl.when(leaf)
            def _():
                up(a, u).wait_send()

            @pl.when(inner)
            def _():
                across(a, u).wait_send()
                down(a, u).wait_send()
    loop(0, n_half * n_pieces, sends)


def mlp(o_part, hidden, mlp_norm, w_o, w_gate, w_up, w_down):
    n_blk, blk_rows, width = o_part.shape
    n_steps, n_batch, d_model = hidden.shape
    n_half = 2
    n_rows = blk_rows // n_half
    n_pieces = d_model // PIECE
    n_chunks = 4
    crows = blk_rows // n_chunks
    ffn = w_gate.shape[1]
    vmem = pl.BlockSpec(memory_space=pltpu.VMEM)
    hbm = pl.BlockSpec(memory_space=pl.ANY)
    dma = pltpu.SemaphoreType.DMA
    n_u = n_half * n_pieces
    piece = (n_u, n_rows, PIECE)
    return pl.pallas_call(
        mlp_kernel,
        out_shape=jax.ShapeDtypeStruct(hidden.shape, BF16),
        in_specs=[hbm, hbm, vmem, hbm, hbm, hbm, hbm],
        out_specs=vmem,
        scratch_shapes=[
            pltpu.VMEM((n_half, n_rows, d_model), BF16),
            pltpu.VMEM(w_o.shape, BF16), pltpu.VMEM(w_gate.shape, BF16),
            pltpu.VMEM(w_up.shape, BF16), pltpu.VMEM(w_down.shape, BF16),
            pltpu.VMEM((2, blk_rows, width), F32), pltpu.VMEM((2, n_chunks, crows, width), F32),
            pltpu.VMEM((n_chunks, crows, width), F32), pltpu.VMEM((n_chunks, crows, width), F32),
            pltpu.VMEM((n_half, n_rows, w_o.shape[0]), BF16),
            pltpu.VMEM((2,) + piece, F32), pltpu.VMEM((2,) + piece, F32),
            pltpu.VMEM((2,) + piece, F32), pltpu.VMEM((2,) + piece, F32),
            pltpu.VMEM(piece, F32), pltpu.VMEM((n_half, n_rows, d_model), BF16), pltpu.VMEM((n_half, n_rows, ffn), BF16),
            pltpu.VMEM(piece, F32), pltpu.VMEM(piece, F32), pltpu.VMEM((2,) + piece, F32),
            dma((n_half, n_steps)), dma((4,)), dma((2,)),
            dma((2, n_chunks)), dma((2, n_chunks)), dma((n_chunks,)), dma((n_chunks,)),
            dma((2, n_u)), dma((2, n_u)), dma((2, n_u)), dma((2, n_u)), dma((2, n_u)), dma((2, n_u)),
            dma((n_u,)), dma((n_u,)), dma((2, n_u)), dma((2, n_u)),
        ],
        compiler_params=pltpu.CompilerParams(vmem_limit_bytes=VMEM_LIMIT, collective_id=0, has_side_effects=True),
        name="combine_mlp",
    )(o_part, hidden, mlp_norm, w_o, w_gate, w_up, w_down)


def solution(mesh):
    cache_spec = P('dp', 'sp', 'tp', None)
    col_spec = P(None, 'tp')
    row_spec = P('tp', None)
    in_specs = (P(None, 'dp', None), P('dp'), cache_spec, cache_spec, col_spec, col_spec, col_spec, row_spec,
                col_spec, col_spec, row_spec, P(), P(), P(), P())
    out_specs = (P(None, 'dp', None), cache_spec, cache_spec)

    def shard_body(hidden, start_pos, k_cache, v_cache, w_q, w_k, w_v, w_o, w_gate, w_up, w_down, attn_norm, mlp_norm, q_gain, k_gain):
        n_steps, n_batch, d_model = hidden.shape
        _, seq, kv, hd = k_cache.shape
        half = np.arange(hd // 2)
        freq = ROPE_BASE ** (-half * (2.0 / hd))
        freq = jnp.asarray(np.concatenate([freq, freq])[None], F32)
        o_part, k_out, v_out = attention(
            start_pos, hidden.reshape(-1, d_model), freq, attn_norm.reshape(-1, 128), q_gain[None], k_gain[None],
            w_q, w_k, w_v, k_cache.reshape(n_batch, seq * kv, hd), v_cache.reshape(n_batch, seq * kv, hd))
        n_sp = 4
        out = mlp(o_part.reshape(n_sp, -1, o_part.shape[1]), hidden, mlp_norm.reshape(-1, 128), w_o, w_gate, w_up, w_down)
        return out, k_out.reshape(k_cache.shape), v_out.reshape(v_cache.shape)

    return jax.shard_map(shard_body, mesh=mesh, in_specs=in_specs, out_specs=out_specs, check_vma=False)
```
